512 devices in a mesh: member: 2 (over y), lon: 32 (over z), lat: 8 (over x, core).
Axes of the slice: x: 4, y: 2, z: 32, core: 2. Of those that a mesh axis runs over, the one named last changes fastest.
The devices are a block of a 4x8x32 slice.
Arguments:
- tracer: float32 [64, 128, 4096], P('member', 'lat', 'lon'), parts along dimension 0, may hold values from -6 to 6
- velocity: float32 [2, 64, 128, 4096], P(None, 'member', 'lat', 'lon'), parts along dimension 1, may hold values from -0.9 to 0.9
- surface: float32 [256, 4096], P(('member', 'lat'), 'lon'), parts along dimension 0, may hold values from -6 to 6
- transport: float32 [4, 128, 4096], P('member', 'lat', 'lon'), parts along dimension 0, may hold values from -3 to 3
- horiz_mixing: float32 [64], P('member'), parts along dimension 0, may hold values from 0.03 to 0.2
- vert_mixing: float32 [62], P('member'), parts along dimension 0, may hold values from 0.3 to 30
- levels: int32 [128, 4096], P('lat', 'lon'), may hold values from 0 to 32, as said below
- land_tiles: int32 [8, 32], P('lat', 'lon'), may hold values 0 or 1
- fold_pair: int32 [4096], P('lon'), may hold values from 0 to 4095, as said below
Outputs:
- tracer_new: float32 [64, 128, 4096], P('member', 'lat', 'lon'), parts along dimension 0
- surface_new: float32 [256, 4096], P(('member', 'lat'), 'lon'), parts along dimension 0
- transport_new: float32 [4, 128, 4096], P('member', 'lat', 'lon'), parts along dimension 0
The draws below stay inside these ranges and needn't reach their ends.
There are 2 independent parts, one for each index of `member`. The reference program is written for one: setup_inputs(seed, part) draws one part's arguments, and reference() takes and returns one part's arrays. A program takes and returns all parts, laid end to end along the dimension named above; an argument that names none is the same for every part. Nothing has to cross between parts.
Inputs may be any that keep to these rules, and one draw needn't show every extreme that they name: 0 marks a land cell, otherwise the count of sea levels. The fold pairing is a reflection: fold_pair[i] = (p - i) mod 4096 for one p in 0..4095, so fold_pair[fold_pair[i]] = i.
All inputs are finite; a program needn't handle non-finite values. No bound on the sum of `land_tiles` on one device may be relied on, other than what follows from the above.
Results may differ from the reference program's by a relative error of at most 0.00002.
Values sent between devices are 32-bit elements; how exact they have to be, the bound alone decides.
No kernel may reach another device: no remote copies, remote signals or barrier semaphores. Data moves between devices by JAX's collectives and lax.ppermute only.
A program may use at most 64 MiB of HBM per device.

```python
import math
import jax
import jax.numpy as jnp

K = 32
SUB = 12
CLAT = 16
CLON = 128
NLAT = 128
NLON = 4096
N_LON = 32
N_LAT = 8


def draw_levels(key, part):
    land_key = jax.random.fold_in(key, 11)
    depth_key = jax.random.fold_in(key, 12)
    land_cells = jax.random.randint(land_key, (NLAT, NLON), 0, 5) == 0
    depth_draw = jax.random.randint(depth_key, (NLAT, NLON), 1, K + 1)
    return jnp.where(land_cells, 0, depth_draw).astype(jnp.int32)


def draw_fold_pair(key, part):
    pivot_key = jax.random.fold_in(key, 21)
    pivot_col = jax.random.randint(pivot_key, (), 0, NLON)
    return jnp.mod(pivot_col - jnp.arange(NLON, dtype=jnp.int32), NLON).astype(jnp.int32)


def set_ends(result, own_key, low, top_value):
    longest = result.shape.index(max(result.shape))
    spots = []
    for shift in (0, 1):
        where = [jax.random.randint(jax.random.fold_in(own_key, axis), (), 0, length) for axis, length in enumerate(result.shape)]
        where[longest] = (where[longest] + shift) % result.shape[longest]
        spots.append(tuple(where))
    return result.at[spots[0]].set(low).at[spots[1]].set(top_value)


def shard_levels(rng, shape, shards, least, top_value):
    loudness = 1.0
    for position, blocks in shards:
        draws = jax.random.uniform(jax.random.fold_in(jax.random.fold_in(rng, 6), position), (blocks,), jnp.float32, least / len(shards), top_value / len(shards))
        loudness = loudness * jnp.repeat(jnp.exp(draws), shape[position] // blocks).reshape((-1,) + (1,) * (len(shape) - 1 - position))
    return loudness


def noise(stream_key, dims, spread, reach, pieces=(), kind=jnp.bfloat16):
    result = spread * jax.random.normal(stream_key, dims, jnp.float32)
    if pieces:
        result = result * shard_levels(stream_key, dims, pieces, -0.22, 0.18)
    return jnp.clip(result, -reach, reach).astype(kind)


def setup_inputs(seed: int = 0, part: int = 0) -> dict:
    arg_keys = jax.random.split(jax.random.key(seed), 10)
    own_keys = jax.random.split(jax.random.fold_in(arg_keys[9], part), 10)
    return {
        "tracer": noise(own_keys[0], (K, NLAT, NLON), 1.0, 6.0, ((1, 8), (2, 32)), jnp.float32),
        "velocity": noise(own_keys[1], (2, K, NLAT, NLON), 0.15, 0.9, ((2, 8), (3, 32)), jnp.float32),
        "surface": noise(own_keys[2], (NLAT, NLON), 1.0, 6.0, ((0, 8), (1, 32)), jnp.float32),
        "transport": noise(own_keys[3], (2, NLAT, NLON), 0.5, 3.0, ((1, 8), (2, 32)), jnp.float32),
        "horiz_mixing": jnp.clip(jnp.exp(jax.random.uniform(own_keys[4], (K,), jnp.float32, math.log(0.03), math.log(0.2))), 0.03, 0.2),
        "vert_mixing": jnp.clip(jnp.exp(jax.random.uniform(own_keys[5], (K - 1,), jnp.float32, math.log(0.3), math.log(30.0))), 0.3, 30.0),
        "levels": draw_levels(jax.random.fold_in(arg_keys[9], 71), part),
        "land_tiles": set_ends((jax.random.randint(arg_keys[7], (N_LAT, N_LON), 0, 4) < 1).astype(jnp.int32), jax.random.fold_in(arg_keys[7], 1), 0, 1),
        "fold_pair": draw_fold_pair(jax.random.fold_in(arg_keys[9], 71), part),
    }


fb_step = 0.6
drag_rate = 0.02


def east_of(field):
    return jnp.roll(field, -1, axis=-1)


def west_of(field):
    return jnp.roll(field, 1, axis=-1)


def north_of(field, fold_pair):
    top_row = jnp.take(field[..., -1:, :], fold_pair, axis=-1)
    return jnp.concatenate([field[..., 1:, :], top_row], axis=-2)


def south_of(field):
    return jnp.concatenate([jnp.zeros_like(field[..., :1, :]), field[..., :-1, :]], axis=-2)


def face_flux(near_side, far_side, wet_near, wet_far, vel_near, vel_far, mixing):
    return wet_near * wet_far * (mixing * (far_side - near_side) - 0.25 * (vel_near + vel_far) * (near_side + far_side))


def thomas(stepped, coupling):
    depth_count = stepped.shape[0]
    primes = []
    sweeps = []
    for depth_idx in range(depth_count):
        diagonal_term = jnp.ones_like(stepped[depth_idx])
        if depth_idx > 0:
            diagonal_term = diagonal_term + coupling[depth_idx - 1]
        if depth_idx < depth_count - 1:
            diagonal_term = diagonal_term + coupling[depth_idx]
        if depth_idx > 0:
            pivot_term = diagonal_term + coupling[depth_idx - 1] * primes[depth_idx - 1]
            reduced = (stepped[depth_idx] + coupling[depth_idx - 1] * sweeps[depth_idx - 1]) / pivot_term
        else:
            pivot_term = diagonal_term
            reduced = stepped[depth_idx] / pivot_term
        if depth_idx < depth_count - 1:
            primes.append(-coupling[depth_idx] / pivot_term)
        else:
            primes.append(jnp.zeros_like(reduced))
        sweeps.append(reduced)
    solved = [None] * depth_count
    solved[depth_count - 1] = sweeps[depth_count - 1]
    for depth_idx in range(depth_count - 2, -1, -1):
        solved[depth_idx] = sweeps[depth_idx] - primes[depth_idx] * solved[depth_idx + 1]
    return jnp.stack(solved)


def reference(tracer, velocity, surface, transport, horiz_mixing, vert_mixing, levels, land_tiles, fold_pair):
    tile_land = jnp.repeat(jnp.repeat(land_tiles, CLAT, axis=0), CLON, axis=1)
    depth_levels = (levels * (1 - tile_land)).astype(jnp.int32)
    level_real = depth_levels.astype(jnp.float32)
    sea_cells = (depth_levels > 0).astype(jnp.float32)
    wet = (jnp.arange(K, dtype=jnp.int32)[:, None, None] < depth_levels[None]).astype(jnp.float32)

    mixing = horiz_mixing[:, None, None]
    zonal_vel = velocity[0]
    merid_vel = velocity[1]
    flux_east = face_flux(tracer, east_of(tracer), wet, east_of(wet), zonal_vel, east_of(zonal_vel), mixing)
    flux_north = face_flux(tracer, north_of(tracer, fold_pair), wet, north_of(wet, fold_pair), merid_vel, north_of(merid_vel, fold_pair), mixing)
    stepped = wet * (tracer + ((flux_east - west_of(flux_east)) + (flux_north - south_of(flux_north))))
    coupling = vert_mixing[:, None, None] * wet[1:]
    tracer_new = thomas(stepped, coupling)

    zonal_mask = sea_cells * east_of(sea_cells)
    zonal_depth = (level_real + east_of(level_real)) / (2.0 * K)
    merid_mask = sea_cells * north_of(sea_cells, fold_pair)
    merid_depth = (level_real + north_of(level_real, fold_pair)) / (2.0 * K)

    height = surface
    zonal = transport[0]
    merid = transport[1]
    for substep in range(SUB):
        divergence = (zonal - west_of(zonal)) + (merid - south_of(merid))
        height = (height - fb_step * divergence) * sea_cells
        east_vals = east_of(height)
        north_vals = north_of(height, fold_pair)
        zonal = (zonal * (1.0 - drag_rate) - fb_step * zonal_depth * (east_vals - height)) * zonal_mask
        merid = (merid * (1.0 - drag_rate) - fb_step * merid_depth * (north_vals - height)) * merid_mask
    return tracer_new, height, jnp.stack([zonal, merid])
```

```python
import functools

import jax
import jax.numpy as jnp
from jax import lax
from jax.experimental import pallas as pl
from jax.experimental.pallas import tpu as pltpu
from jax.sharding import PartitionSpec as P

SUB = 12
fb_step = 0.6
drag_rate = 0.02
EDGE = 16
F32 = jnp.float32


def lanes_of(shape):
    return lax.broadcasted_iota(jnp.int32, shape, 1)


def rows_of(shape):
    return lax.broadcasted_iota(jnp.int32, shape, 0)


def roll(x, shift, axis):
    return pltpu.roll(x, shift % x.shape[axis], axis)


def pack_kernel(land, tracer, velocity, surface, transport, levels, up, down, cols):
    depth, rows, width = tracer.shape
    real = (levels[...] * (1 - land[0, 0])).astype(F32)
    for out, row in ((up, rows - 1), (down, 0)):
        out[0:rows] = surface[...]
        out[rows : 2 * rows] = transport[0]
        out[2 * rows : 3 * rows] = transport[1]
        out[3 * rows : 4 * rows] = real
        for k in range(depth):
            out[4 * rows + k : 4 * rows + k + 1] = tracer[k, row : row + 1]
            at = 4 * rows + depth + k
            out[at : at + 1] = velocity[1, k, row : row + 1]
    lane = lanes_of((8, width))
    first = jnp.zeros((8, width), F32)
    last = jnp.zeros((8, width), F32)
    spot = 0
    for field in range(2):
        for k in range(depth):
            for half in range(0, rows, 8):
                part = tracer[k, half : half + 8] if field == 0 else velocity[0, k, half : half + 8]
                first = jnp.where(lane == spot, part[:, :1], first)
                last = jnp.where(lane == spot, part[:, width - 1 :], last)
                spot += 1
    cols[0:8] = first
    cols[8:16] = last


def edge_kernel(place, up, south, north, cols, main, extra, eastward, westward):
    rows = up.shape[0] // 8
    width = up.shape[1]
    groups = width // EDGE
    lane = lanes_of((8, width)) // EDGE
    n = 0
    east = west = None
    for field in range(4):
        for block in (south, up, north):
            for half in range(0, rows, 8):
                group = n % groups
                x = block[field * rows + half : field * rows + half + 8]
                to_east = roll(x, EDGE * group - (width - EDGE), 1)
                to_west = roll(x, EDGE * group, 1)
                if group == 0:
                    east, west = to_east, to_west
                else:
                    east = jnp.where(lane == group, to_east, east)
                    west = jnp.where(lane == group, to_west, west)
                n += 1
                if n % groups == 0:
                    at = 8 * (n // groups - 1)
                    eastward[at : at + 8] = east
                    westward[at : at + 8] = west
    at = 8 * (n // groups)
    eastward[at : at + 8] = cols[8:16]
    westward[at : at + 8] = cols[0:8]
    at, size = at + 8, main.shape[0]
    is_first = jnp.full((size, width), place[2], jnp.int32) == 0
    center = jnp.where(is_first, extra[...], main[...])
    eastward[at : at + size] = center
    westward[at : at + size] = center
    westward[at + size : at + 2 * size] = main[...]


def final_kernel(
    n_lon, place, hmix, vmix, tracer, velocity, up, down, south, north, cols, from_west, from_east, main, extra,
    tracer_out, surface_out, transport_out,
    north_own, north_far, seam_own, seam_far, north_rows, primes,
):
    depth, rows, width = tracer.shape
    groups = width // EDGE
    lane8 = lanes_of((8, width))
    half_way = width // 2
    flat = 4 * rows

    def far_tile(n):
        at, group = 8 * (n // groups), n % groups
        east = roll(from_east[at : at + 8], -EDGE * group, 1)
        west = roll(from_west[at : at + 8], (width - EDGE) - EDGE * group, 1)
        return jnp.where(lane8 < half_way, east, west)

    def far_block(field, block):
        first = (field * 3 + block) * (rows // 8)
        return jnp.concatenate([far_tile(first + i) for i in range(rows // 8)], axis=0)

    def shifted(own, far, by):
        lane = lanes_of(own.shape)
        edge = width - 1 if by < 0 else 0
        a, b = roll(own, by, 1), roll(far, by, 1)
        return jnp.where(lane == edge, b, a), jnp.where(lane == edge, a, b)

    at_top = place[0] == 1

    @pl.when(jnp.logical_not(at_top))
    def _():
        north_own[...] = north[0:flat]
        for field in range(4):
            north_far[field * rows : (field + 1) * rows] = far_block(field, 2)
        seam_own[...] = roll(up[3 * rows - 8 : 3 * rows], 1, 0)
        seam_far[...] = roll(far_tile((2 * 3 + 1) * (rows // 8) + rows // 8 - 1), 1, 0)
        north_rows[...] = north[flat : flat + 2 * depth]

    @pl.when(at_top)
    def _():
        turn = place[1]
        small = jnp.full((8, width), turn, jnp.int32) < half_way
        index = (turn - lane8) & (width - 1)
        less = lane8 <= turn
        back = 7 - rows_of((8, width))

        lon = jnp.full((8, width), place[2], jnp.int32)
        is_first, is_last, is_before = lon == 0, lon == n_lon - 1, lon == n_lon - 2
        sent = 4 * 3 * rows // groups + 8
        size = main.shape[0]

        def pulled(at):
            west = from_west[sent + at : sent + at + 8]
            east = from_east[sent + at : sent + at + 8]
            further = from_east[sent + size + at : sent + size + at + 8]
            g0, g1, g2 = (
                jnp.take_along_axis(x, index, axis=1, mode="promise_in_bounds")
                for x in (
                    jnp.where(is_first, main[at : at + 8], west),
                    jnp.where(
                        is_last,
                        further,
                        jnp.where(is_first, extra[at : at + 8], main[at : at + 8]),
                    ),
                    jnp.where(is_before, extra[at : at + 8], east),
                )
            )
            own = jnp.where(less, jnp.where(small, g0, g1), jnp.where(small, g1, g2))
            return own, g0, g1, g2

        def turned(x):
            return jnp.take_along_axis(x, back, axis=0, mode="promise_in_bounds")

        for field in range(4):
            own, far = [], []
            for half in range(rows - 8, -8, -8):
                mine, g0, g1, g2 = pulled(field * rows + half)
                low = jnp.where(jnp.logical_and(less, small), g1, g2)
                high = jnp.where(jnp.logical_or(less, small), g0, g1)
                own.append(turned(mine))
                far.append(turned(jnp.where(lane8 < half_way, low, high)))
            own, far = jnp.concatenate(own, axis=0), jnp.concatenate(far, axis=0)
            if field == 1:
                own, far = shifted(-own, -far, -1)
            if field == 2:
                seam_own[...] = -own[:8]
                seam_far[...] = -far[:8]
                own, far = roll(-own, -1, 0), roll(-far, -1, 0)
            north_own[field * rows : (field + 1) * rows] = own
            north_far[field * rows : (field + 1) * rows] = far
        for at in range(0, 2 * depth, 8):
            north_rows[at : at + 8] = pulled(flat + at)[0]

    def window(field):
        at = slice(field * rows, (field + 1) * rows)
        own = jnp.concatenate([south[at], up[at], north_own[at]], axis=0)
        far = jnp.concatenate([far_block(field, 0), far_block(field, 1), north_far[at]], axis=0)
        return own, far

    eta, far_eta = window(0)
    u, far_u = window(1)
    v, far_v = window(2)
    level, far_level = window(3)
    seam, far_seam = seam_own[...], seam_far[...]
    total = 3 * rows

    def sea_of(x):
        return (x > 0).astype(F32)

    sea, far_sea = sea_of(level), sea_of(far_level)
    east_sea, east_far_sea = shifted(sea, far_sea, -1)
    east_level, east_far_level = shifted(level, far_level, -1)
    scale = 2.0 * depth
    zmask, far_zmask = sea * east_sea, far_sea * east_far_sea
    zdepth = fb_step * ((level + east_level) / scale)
    far_zdepth = fb_step * ((far_level + east_far_level) / scale)
    mmask, far_mmask = sea * roll(sea, -1, 0), far_sea * roll(far_sea, -1, 0)
    mdepth = fb_step * ((level + roll(level, -1, 0)) / scale)
    far_mdepth = fb_step * ((far_level + roll(far_level, -1, 0)) / scale)
    cut = 2 * rows

    def below(x):
        return roll(x, 1, 0)[cut : cut + 8]

    seam_mask, far_seam_mask = below(mmask), below(far_mmask)
    seam_depth, far_seam_depth = below(mdepth), below(far_mdepth)
    row8 = rows_of((8, width))

    def south_of(x, line):
        moved = roll(x, 1, 0)
        fixed = jnp.where(row8 == 0, line, moved[cut : cut + 8])
        return jnp.concatenate([moved[:cut], fixed, moved[cut + 8 :]], axis=0)

    keep = 1.0 - drag_rate
    for _ in range(SUB):
        west_u, west_far_u = shifted(u, far_u, 1)
        div = (u - west_u) + (v - south_of(v, seam))
        far_div = (far_u - west_far_u) + (far_v - south_of(far_v, far_seam))
        eta = (eta - fb_step * div) * sea
        far_eta = (far_eta - fb_step * far_div) * far_sea
        east, far_east = shifted(eta, far_eta, -1)
        u = (u * keep - zdepth * (east - eta)) * zmask
        far_u = (far_u * keep - far_zdepth * (far_east - far_eta)) * far_zmask
        rise = eta[cut : cut + 8] - below(eta)
        far_rise = far_eta[cut : cut + 8] - below(far_eta)
        seam = (seam * keep - seam_depth * rise) * seam_mask
        far_seam = (far_seam * keep - far_seam_depth * far_rise) * far_seam_mask
        v = (v * keep - mdepth * (roll(eta, -1, 0) - eta)) * mmask
        far_v = (far_v * keep - far_mdepth * (roll(far_eta, -1, 0) - far_eta)) * far_mmask
    mid = slice(rows, 2 * rows)
    surface_out[...] = eta[mid]
    transport_out[0] = u[mid]
    transport_out[1] = v[mid]

    def face(near, beyond, wet_near, wet_beyond, vel_near, vel_beyond, mixing):
        flux = mixing * (beyond - near) - 0.25 * (vel_near + vel_beyond) * (near + beyond)
        return jnp.where(jnp.logical_and(wet_near, wet_beyond), flux, 0.0)

    level_row = rows_of((depth, width)).astype(F32)
    mix_rows = jnp.zeros((depth, width), F32)
    for k in range(depth):
        mix_rows = jnp.where(level_row == k, hmix[k], mix_rows)
    top, bottom = level[2 * rows - 1 : 2 * rows], level[rows : rows + 1]
    flux_top = face(
        up[flat : flat + depth],
        north_rows[0:depth],
        level_row < top,
        level_row < level[2 * rows : 2 * rows + 1],
        up[flat + depth : flat + 2 * depth],
        north_rows[depth : 2 * depth],
        mix_rows,
    )
    flux_bottom = face(
        south[flat : flat + depth],
        down[flat : flat + depth],
        level_row < level[rows - 1 : rows],
        level_row < bottom,
        south[flat + depth : flat + 2 * depth],
        down[flat + depth : flat + 2 * depth],
        mix_rows,
    )
    parts = rows // 8
    level_lane = ((lane8 & (parts * depth - 1)) // parts).astype(F32)
    mix_lanes = jnp.zeros((8, width), F32)
    for k in range(depth):
        mix_lanes = jnp.where(level_lane == k, hmix[k], mix_lanes)
    here, far_here = level[mid], far_level[mid]

    def column(x, at):
        packed = jnp.broadcast_to(x[:8, at : at + 1], (8, width))
        for i in range(1, parts):
            packed = jnp.where(lane8 % parts == i, x[8 * i : 8 * i + 8, at : at + 1], packed)
        return packed

    def side(near, beyond, level_near, level_beyond):
        return face(
            near,
            beyond,
            level_lane < level_near,
            level_lane < level_beyond,
            roll(near, -half_way, 1),
            roll(beyond, -half_way, 1),
            mix_lanes,
        )

    spot = 8 * (4 * 3 * parts // groups)
    flux_right = side(
        cols[8:16], from_east[spot : spot + 8], column(here, width - 1), column(far_here, 0)
    )
    flux_left = side(
        from_west[spot : spot + 8], cols[0:8], column(far_here, width - 1), column(here, 0)
    )

    lane = lanes_of((rows, width))
    row = rows_of((rows, width))
    here_east = roll(here, -1, 1)
    here_north = roll(here, -1, 0)

    def spread(x, k):
        return jnp.concatenate(
            [jnp.broadcast_to(x[:, parts * k + i : parts * k + i + 1], (8, width)) for i in range(parts)],
            axis=0,
        )

    sweep = prime = link = None
    for k in range(depth):
        field, zonal, merid = tracer[k], velocity[0, k], velocity[1, k]
        wet = here > k
        mixing = hmix[k]
        east_flux = face(
            field, roll(field, -1, 1), wet, here_east > k, zonal, roll(zonal, -1, 1), mixing
        )
        east_flux = jnp.where(lane == width - 1, spread(flux_right, k), east_flux)
        west_flux = jnp.where(lane == 0, spread(flux_left, k), roll(east_flux, 1, 1))
        north_flux = face(
            field, roll(field, -1, 0), wet, here_north > k, merid, roll(merid, -1, 0), mixing
        )
        north_flux = jnp.where(row == rows - 1, flux_top[k : k + 1], north_flux)
        south_flux = jnp.where(row == 0, flux_bottom[k : k + 1], roll(north_flux, 1, 0))
        stepped = jnp.where(
            wet, field + ((east_flux - west_flux) + (north_flux - south_flux)), 0.0
        )
        diagonal = jnp.ones_like(stepped)
        if k > 0:
            diagonal = diagonal + link
        if k < depth - 1:
            next_link = jnp.where(here > k + 1, vmix[k], 0.0)
            diagonal = diagonal + next_link
        if k > 0:
            diagonal = diagonal + link * prime
            stepped = stepped + link * sweep
        inverse = 1.0 / diagonal
        sweep = stepped * inverse
        tracer_out[k] = sweep
        if k < depth - 1:
            prime = -next_link * inverse
            primes[k] = prime
            link = next_link
    solved = sweep
    for k in range(depth - 2, -1, -1):
        solved = tracer_out[k] - primes[k] * solved
        tracer_out[k] = solved


def shards(
    tracer, velocity, surface, transport, horiz_mixing, vert_mixing, levels, land_tiles, fold_pair,
    *, n_lon, n_lat, interpret,
):
    depth, rows, width = tracer.shape
    smem = pl.BlockSpec(memory_space=pltpu.SMEM)
    vmem = pl.BlockSpec(memory_space=pltpu.VMEM)
    call = functools.partial(pl.pallas_call, interpret=interpret)

    def like(*shape):
        return jax.ShapeDtypeStruct(shape, F32)

    stack = 4 * rows + 2 * depth
    up, down, cols = call(
        pack_kernel,
        out_shape=(like(stack, width), like(stack, width), like(16, width)),
        in_specs=[smem] + [vmem] * 5,
        out_specs=(vmem,) * 3,
        name="pack",
    )(land_tiles, tracer, velocity, surface, transport, levels)

    south = lax.ppermute(up, "lat", [(i, i + 1) for i in range(n_lat - 1)])
    north = lax.ppermute(down, "lat", [(i + 1, i) for i in range(n_lat - 1)])

    lon = lax.axis_index("lon")
    pivot = (fold_pair[0] + width * lon) % (width * n_lon)
    turn = pivot % width
    tile = (pivot // width - (turn < width // 2).astype(jnp.int32)) % n_lon

    def branch(shift):
        def pairs(routes):
            return [(s % n_lon * n_lat + n_lat - 1, t * n_lat + n_lat - 1) for s, t in routes]

        most = [(shift + 1, 0)] + [(shift - t, t) for t in range(1, n_lon - 1)]
        rest = [(shift, 0), (shift + 1, n_lon - 2)]
        return lambda x: (
            lax.ppermute(x, ("lon", "lat"), pairs(most)),
            lax.ppermute(x, ("lon", "lat"), pairs(rest)),
        )

    main, extra = lax.switch(tile, [branch(shift) for shift in range(n_lon)], up)

    at_top = (lax.axis_index("lat") == n_lat - 1).astype(jnp.int32)
    place = jnp.stack([at_top, turn, lon])
    edge_rows = 4 * 3 * rows * EDGE // width + 8
    eastward, westward = call(
        edge_kernel,
        out_shape=(like(edge_rows + stack, width), like(edge_rows + 2 * stack, width)),
        in_specs=[smem] + [vmem] * 6,
        out_specs=(vmem,) * 2,
        name="edge",
    )(place, up, south, north, cols, main, extra)
    from_west = lax.ppermute(eastward, "lon", [(i, (i + 1) % n_lon) for i in range(n_lon)])
    from_east = lax.ppermute(westward, "lon", [((i + 1) % n_lon, i) for i in range(n_lon)])

    return call(
        functools.partial(final_kernel, n_lon),
        out_shape=(like(depth, rows, width), like(rows, width), like(2, rows, width)),
        in_specs=[smem] * 3 + [vmem] * 11,
        out_specs=(vmem,) * 3,
        scratch_shapes=[
            pltpu.VMEM((4 * rows, width), F32),
            pltpu.VMEM((4 * rows, width), F32),
            pltpu.VMEM((8, width), F32),
            pltpu.VMEM((8, width), F32),
            pltpu.VMEM((2 * depth, width), F32),
            pltpu.VMEM((depth, rows, width), F32),
        ],
        name="final",
    )(
        place, horiz_mixing, vert_mixing, tracer, velocity, up, down, south, north, cols,
        from_west, from_east, main, extra,
    )


def solution(mesh, interpret=False):
    return jax.shard_map(
        functools.partial(
            shards, n_lon=mesh.shape["lon"], n_lat=mesh.shape["lat"], interpret=interpret
        ),
        mesh=mesh,
        in_specs=(
            P("member", "lat", "lon"),
            P(None, "member", "lat", "lon"),
            P(("member", "lat"), "lon"),
            P("member", "lat", "lon"),
            P("member"),
            P("member"),
            P("lat", "lon"),
            P("lat", "lon"),
            P("lon"),
        ),
        out_specs=(
            P("member", "lat", "lon"),
            P(("member", "lat"), "lon"),
            P("member", "lat", "lon"),
        ),
        check_vma=False,
    )
```

```python
import functools

import jax
import jax.numpy as jnp
from jax import lax
from jax.experimental import pallas as pl
from jax.experimental.pallas import tpu as pltpu
from jax.sharding import PartitionSpec as P


SUB = 12
fb_step = 0.6
drag_rate = 0.02
EDGE = 16
F32 = jnp.float32


def lanes_of(shape):
    return lax.broadcasted_iota(jnp.int32, shape, 1)


def rows_of(shape):
    return lax.broadcasted_iota(jnp.int32, shape, 0)


def roll(x, shift, axis):
    return pltpu.roll(x, shift % x.shape[axis], axis)


def pack_kernel(land, tracer, velocity, surface, transport, levels, up, down, cols):
    depth, rows, width = tracer.shape
    real = (levels[...] * (1 - land[...])).astype(F32)
    for out, row in ((up, rows - 1), (down, 0)):
        out[0:rows] = surface[...]
        out[rows : 2 * rows] = transport[0]
        out[2 * rows : 3 * rows] = transport[1]
        out[3 * rows : 4 * rows] = real
        for k in range(depth):
            out[4 * rows + k : 4 * rows + k + 1] = tracer[k, row : row + 1]
            at = 4 * rows + depth + k
            out[at : at + 1] = velocity[1, k, row : row + 1]
    lane = lanes_of((8, width))
    first = jnp.zeros((8, width), F32)
    last = jnp.zeros((8, width), F32)
    spot = 0
    for field in range(2):
        for k in range(depth):
            for half in range(0, rows, 8):
                part = tracer[k, half : half + 8] if field == 0 else velocity[0, k, half : half + 8]
                first = jnp.where(lane == spot, part[:, :1], first)
                last = jnp.where(lane == spot, part[:, width - 1 :], last)
                spot += 1
    cols[0:8] = first
    cols[8:16] = last


def edge_kernel(lon, up, south, north, cols, main, extra, eastward, westward):
    rows = up.shape[0] // 8
    width = up.shape[1]
    groups = width // EDGE
    lane = lanes_of((8, width)) // EDGE
    n = 0
    east = west = None
    for field in range(4):
        for block in (south, up, north):
            for half in range(0, rows, 8):
                group = n % groups
                x = block[field * rows + half : field * rows + half + 8]
                to_east = roll(x, EDGE * group - (width - EDGE), 1)
                to_west = roll(x, EDGE * group, 1)
                if group == 0:
                    east, west = to_east, to_west
                else:
                    east = jnp.where(lane == group, to_east, east)
                    west = jnp.where(lane == group, to_west, west)
                n += 1
                if n % groups == 0:
                    at = 8 * (n // groups - 1)
                    eastward[at : at + 8] = east
                    westward[at : at + 8] = west
    at = 8 * (n // groups)
    eastward[at : at + 8] = cols[8:16]
    westward[at : at + 8] = cols[0:8]
    at, size = at + 8, main.shape[0]
    is_first = jnp.full((size, width), lon[0], jnp.int32) == 0
    eastward[at : at + size] = jnp.where(is_first, extra[...], main[...])
    westward[at : at + size] = main[...]
    westward[at + size : at + 2 * size] = extra[...]


def final_kernel(
    n_lon, lon_ref, turn_ref, top_ref, hmix, vmix, tracer, velocity, up, down, south, north, cols, from_west, from_east, main, extra,
    tracer_out, surface_out, transport_out,
    north_own, north_far, seam_own, seam_far, north_rows, primes,
):
    depth, rows, width = tracer.shape
    groups = width // EDGE
    lane8 = lanes_of((8, width))
    half_way = width // 2
    flat = 4 * rows

    def far_tile(n):
        at, group = 8 * (n // groups), n % groups
        east = roll(from_east[at : at + 8], -EDGE * group, 1)
        west = roll(from_west[at : at + 8], (width - EDGE) - EDGE * group, 1)
        return jnp.where(lane8 < half_way, east, west)

    def far_block(field, block):
        first = (field * 3 + block) * (rows // 8)
        return jnp.concatenate([far_tile(first + i) for i in range(rows // 8)], axis=0)

    def shifted(own, far, by):
        lane = lanes_of(own.shape)
        edge = width - 1 if by < 0 else 0
        a, b = roll(own, by, 1), roll(far, by, 1)
        return jnp.where(lane == edge, b, a), jnp.where(lane == edge, a, b)

    at_top = top_ref[0] == 1

    @pl.when(jnp.logical_not(at_top))
    def _():
        north_own[...] = north[0:flat]
        for field in range(4):
            north_far[field * rows : (field + 1) * rows] = far_block(field, 2)
        seam_own[...] = roll(up[3 * rows - 8 : 3 * rows], 1, 0)
        seam_far[...] = roll(far_tile((2 * 3 + 1) * (rows // 8) + rows // 8 - 1), 1, 0)
        north_rows[...] = north[flat : flat + 2 * depth]

    @pl.when(at_top)
    def _():
        turn = turn_ref[0]
        small = jnp.full((8, width), turn, jnp.int32) < half_way
        index = (turn - lane8) & (width - 1)
        less = lane8 <= turn
        back = 7 - rows_of((8, width))

        lon = jnp.full((8, width), lon_ref[0], jnp.int32)
        is_first, is_last = lon == 0, lon == n_lon - 1
        sent = 4 * 3 * rows // groups + 8
        size = main.shape[0]

        def pulled(at):
            mine, other = main[at : at + 8], extra[at : at + 8]
            west = from_west[sent + at : sent + at + 8]
            east = from_east[sent + at : sent + at + 8]
            further = from_east[sent + size + at : sent + size + at + 8]
            g0, g1, g2 = (
                jnp.take_along_axis(x, index, axis=1, mode="promise_in_bounds")
                for x in (
                    jnp.where(is_first, mine, west),
                    jnp.where(is_last, east, jnp.where(is_first, other, mine)),
                    jnp.where(is_last, further, jnp.where(is_first, east, other)),
                )
            )
            own = jnp.where(less, jnp.where(small, g0, g1), jnp.where(small, g1, g2))
            return own, g0, g1, g2

        def turned(x):
            return jnp.take_along_axis(x, back, axis=0, mode="promise_in_bounds")

        for field in range(4):
            own, far = [], []
            for half in range(rows - 8, -8, -8):
                mine, g0, g1, g2 = pulled(field * rows + half)
                low = jnp.where(jnp.logical_and(less, small), g1, g2)
                high = jnp.where(jnp.logical_or(less, small), g0, g1)
                own.append(turned(mine))
                far.append(turned(jnp.where(lane8 < half_way, low, high)))
            own, far = jnp.concatenate(own, axis=0), jnp.concatenate(far, axis=0)
            if field == 1:
                own, far = shifted(-own, -far, -1)
            if field == 2:
                seam_own[...] = -own[:8]
                seam_far[...] = -far[:8]
                own, far = roll(-own, -1, 0), roll(-far, -1, 0)
            north_own[field * rows : (field + 1) * rows] = own
            north_far[field * rows : (field + 1) * rows] = far
        for at in range(0, 2 * depth, 8):
            north_rows[at : at + 8] = pulled(flat + at)[0]

    def window(field):
        at = slice(field * rows, (field + 1) * rows)
        own = jnp.concatenate([south[at], up[at], north_own[at]], axis=0)
        far = jnp.concatenate([far_block(field, 0), far_block(field, 1), north_far[at]], axis=0)
        return own, far

    eta, far_eta = window(0)
    u, far_u = window(1)
    v, far_v = window(2)
    level, far_level = window(3)
    seam, far_seam = seam_own[...], seam_far[...]

    def sea_of(x):
        return (x > 0).astype(F32)

    sea, far_sea = sea_of(level), sea_of(far_level)
    east_sea, east_far_sea = shifted(sea, far_sea, -1)
    east_level, east_far_level = shifted(level, far_level, -1)
    scale = 2.0 * depth
    zmask, far_zmask = sea * east_sea, far_sea * east_far_sea
    zdepth = fb_step * ((level + east_level) / scale)
    far_zdepth = fb_step * ((far_level + east_far_level) / scale)
    mmask, far_mmask = sea * roll(sea, -1, 0), far_sea * roll(far_sea, -1, 0)
    mdepth = fb_step * ((level + roll(level, -1, 0)) / scale)
    far_mdepth = fb_step * ((far_level + roll(far_level, -1, 0)) / scale)
    cut = 2 * rows

    def below(x):
        return roll(x, 1, 0)[cut : cut + 8]

    seam_mask, far_seam_mask = below(mmask), below(far_mmask)
    seam_depth, far_seam_depth = below(mdepth), below(far_mdepth)
    row8 = rows_of((8, width))

    def south_of(x, line):
        moved = roll(x, 1, 0)
        fixed = jnp.where(row8 == 0, line, moved[cut : cut + 8])
        return jnp.concatenate([moved[:cut], fixed, moved[cut + 8 :]], axis=0)

    keep = 1.0 - drag_rate
    for _ in range(SUB):
        west_u, west_far_u = shifted(u, far_u, 1)
        div = (u - west_u) + (v - south_of(v, seam))
        far_div = (far_u - west_far_u) + (far_v - south_of(far_v, far_seam))
        eta = (eta - fb_step * div) * sea
        far_eta = (far_eta - fb_step * far_div) * far_sea
        east, far_east = shifted(eta, far_eta, -1)
        u = (u * keep - zdepth * (east - eta)) * zmask
        far_u = (far_u * keep - far_zdepth * (far_east - far_eta)) * far_zmask
        rise = eta[cut : cut + 8] - below(eta)
        far_rise = far_eta[cut : cut + 8] - below(far_eta)
        seam = (seam * keep - seam_depth * rise) * seam_mask
        far_seam = (far_seam * keep - far_seam_depth * far_rise) * far_seam_mask
        v = (v * keep - mdepth * (roll(eta, -1, 0) - eta)) * mmask
        far_v = (far_v * keep - far_mdepth * (roll(far_eta, -1, 0) - far_eta)) * far_mmask
    mid = slice(rows, 2 * rows)
    surface_out[...] = eta[mid]
    transport_out[0] = u[mid]
    transport_out[1] = v[mid]

    def face(near, beyond, wet_near, wet_beyond, vel_near, vel_beyond, mixing):
        flux = mixing * (beyond - near) - 0.25 * (vel_near + vel_beyond) * (near + beyond)
        return jnp.where(jnp.logical_and(wet_near, wet_beyond), flux, 0.0)

    level_row = rows_of((depth, width)).astype(F32)
    mix_rows = jnp.zeros((depth, width), F32)
    for k in range(depth):
        mix_rows = jnp.where(level_row == k, hmix[k], mix_rows)
    top, bottom = level[2 * rows - 1 : 2 * rows], level[rows : rows + 1]
    flux_top = face(
        up[flat : flat + depth],
        north_rows[0:depth],
        level_row < top,
        level_row < level[2 * rows : 2 * rows + 1],
        up[flat + depth : flat + 2 * depth],
        north_rows[depth : 2 * depth],
        mix_rows,
    )
    flux_bottom = face(
        south[flat : flat + depth],
        down[flat : flat + depth],
        level_row < level[rows - 1 : rows],
        level_row < bottom,
        south[flat + depth : flat + 2 * depth],
        down[flat + depth : flat + 2 * depth],
        mix_rows,
    )
    parts = rows // 8
    level_lane = ((lane8 & (parts * depth - 1)) // parts).astype(F32)
    mix_lanes = jnp.zeros((8, width), F32)
    for k in range(depth):
        mix_lanes = jnp.where(level_lane == k, hmix[k], mix_lanes)
    here, far_here = level[mid], far_level[mid]

    def column(x, at):
        packed = jnp.broadcast_to(x[:8, at : at + 1], (8, width))
        for i in range(1, parts):
            packed = jnp.where(lane8 % parts == i, x[8 * i : 8 * i + 8, at : at + 1], packed)
        return packed

    def side(near, beyond, level_near, level_beyond):
        return face(
            near,
            beyond,
            level_lane < level_near,
            level_lane < level_beyond,
            roll(near, -half_way, 1),
            roll(beyond, -half_way, 1),
            mix_lanes,
        )

    spot = 8 * (4 * 3 * parts // groups)
    flux_right = side(
        cols[8:16], from_east[spot : spot + 8], column(here, width - 1), column(far_here, 0)
    )
    flux_left = side(
        from_west[spot : spot + 8], cols[0:8], column(far_here, width - 1), column(here, 0)
    )

    lane = lanes_of((rows, width))
    row = rows_of((rows, width))
    here_east = roll(here, -1, 1)
    here_north = roll(here, -1, 0)

    def spread(x, k):
        return jnp.concatenate(
            [jnp.broadcast_to(x[:, parts * k + i : parts * k + i + 1], (8, width)) for i in range(parts)],
            axis=0,
        )

    sweep = prime = link = None
    for k in range(depth):
        field, zonal, merid = tracer[k], velocity[0, k], velocity[1, k]
        wet = here > k
        mixing = hmix[k]
        east_flux = face(
            field, roll(field, -1, 1), wet, here_east > k, zonal, roll(zonal, -1, 1), mixing
        )
        east_flux = jnp.where(lane == width - 1, spread(flux_right, k), east_flux)
        west_flux = jnp.where(lane == 0, spread(flux_left, k), roll(east_flux, 1, 1))
        north_flux = face(
            field, roll(field, -1, 0), wet, here_north > k, merid, roll(merid, -1, 0), mixing
        )
        north_flux = jnp.where(row == rows - 1, flux_top[k : k + 1], north_flux)
        south_flux = jnp.where(row == 0, flux_bottom[k : k + 1], roll(north_flux, 1, 0))
        stepped = jnp.where(
            wet, field + ((east_flux - west_flux) + (north_flux - south_flux)), 0.0
        )
        diagonal = jnp.ones_like(stepped)
        if k > 0:
            diagonal = diagonal + link
        if k < depth - 1:
            next_link = jnp.where(here > k + 1, vmix[k], 0.0)
            diagonal = diagonal + next_link
        if k > 0:
            diagonal = diagonal + link * prime
            stepped = stepped + link * sweep
        inverse = 1.0 / diagonal
        sweep = stepped * inverse
        tracer_out[k] = sweep
        if k < depth - 1:
            prime = -next_link * inverse
            primes[k] = prime
            link = next_link
    solved = sweep
    for k in range(depth - 2, -1, -1):
        solved = tracer_out[k] - primes[k] * solved
        tracer_out[k] = solved


def shards(
    tracer, velocity, surface, transport, horiz_mixing, vert_mixing, levels, land_tiles, fold_pair,
    *, n_lon, n_lat, interpret,
):
    depth, rows, width = tracer.shape
    smem = pl.BlockSpec(memory_space=pltpu.SMEM)
    vmem = pl.BlockSpec(memory_space=pltpu.VMEM)
    call = functools.partial(pl.pallas_call, interpret=interpret)

    def like(*shape):
        return jax.ShapeDtypeStruct(shape, F32)

    stack = 4 * rows + 2 * depth
    up, down, cols = call(
        pack_kernel,
        out_shape=(like(stack, width), like(stack, width), like(16, width)),
        in_specs=[vmem] * 6,
        out_specs=(vmem,) * 3,
        name="pack",
    )(land_tiles, tracer, velocity, surface, transport, levels)

    south = lax.ppermute(up, "lat", [(i, i + 1) for i in range(n_lat - 1)])
    north = lax.ppermute(down, "lat", [(i + 1, i) for i in range(n_lat - 1)])

    lon = lax.axis_index("lon")
    pivot = (fold_pair[0] + width * lon) % (width * n_lon)
    turn = pivot % width
    tile = (pivot // width - (turn < width // 2).astype(jnp.int32)) % n_lon

    def fetch(x, shift):
        routes = [(shift + 1, 0)] + [(shift - t, t) for t in range(1, n_lon - 1)]
        pairs = [(s % n_lon * n_lat + n_lat - 1, t * n_lat + n_lat - 1) for s, t in routes]
        return lax.ppermute(x, ("lon", "lat"), pairs)

    def branch(shift):
        return lambda x: (fetch(x, shift), fetch(x, (shift - 1) % n_lon))

    main, extra = lax.switch(tile, [branch(shift) for shift in range(n_lon)], up)

    at_top = (lax.axis_index("lat") == n_lat - 1).astype(jnp.int32)
    lon, turn, at_top = (x.reshape(1) for x in (lon, turn, at_top))
    edge_rows = 4 * 3 * rows * EDGE // width + 8
    eastward, westward = call(
        edge_kernel,
        out_shape=(like(edge_rows + stack, width), like(edge_rows + 2 * stack, width)),
        in_specs=[smem] + [vmem] * 6,
        out_specs=(vmem,) * 2,
        name="edge",
    )(lon, up, south, north, cols, main, extra)
    from_west = lax.ppermute(eastward, "lon", [(i, (i + 1) % n_lon) for i in range(n_lon)])
    from_east = lax.ppermute(westward, "lon", [((i + 1) % n_lon, i) for i in range(n_lon)])

    return call(
        functools.partial(final_kernel, n_lon),
        out_shape=(like(depth, rows, width), like(rows, width), like(2, rows, width)),
        in_specs=[smem] * 5 + [vmem] * 11,
        out_specs=(vmem,) * 3,
        scratch_shapes=[
            pltpu.VMEM((4 * rows, width), F32),
            pltpu.VMEM((4 * rows, width), F32),
            pltpu.VMEM((8, width), F32),
            pltpu.VMEM((8, width), F32),
            pltpu.VMEM((2 * depth, width), F32),
            pltpu.VMEM((depth, rows, width), F32),
        ],
        name="final",
    )(
        lon, turn, at_top, horiz_mixing, vert_mixing, tracer, velocity, up, down, south, north, cols,
        from_west, from_east, main, extra,
    )


def solution(mesh, interpret=False):
    def step(*args):
        return shards(*args, n_lon=mesh.shape["lon"], n_lat=mesh.shape["lat"], interpret=interpret)

    return jax.shard_map(
        step,
        mesh=mesh,
        in_specs=(
            P("member", "lat", "lon"),
            P(None, "member", "lat", "lon"),
            P(("member", "lat"), "lon"),
            P("member", "lat", "lon"),
            P("member"),
            P("member"),
            P("lat", "lon"),
            P("lat", "lon"),
            P("lon"),
        ),
        out_specs=(
            P("member", "lat", "lon"),
            P(("member", "lat"), "lon"),
            P("member", "lat", "lon"),
        ),
        check_vma=False,
    )
```

```python
import functools

import jax
import jax.numpy as jnp
from jax import lax
from jax.experimental import pallas as pl
from jax.experimental.pallas import tpu as pltpu
from jax.sharding import PartitionSpec as P


SUB = 12
fb_step = 0.6
drag_rate = 0.02
EDGE = 16
F32 = jnp.float32


def lanes_of(shape):
    return lax.broadcasted_iota(jnp.int32, shape, 1)


def rows_of(shape):
    return lax.broadcasted_iota(jnp.int32, shape, 0)


def roll(x, shift, axis):
    return pltpu.roll(x, shift % x.shape[axis], axis)


def pack_kernel(land, tracer, velocity, surface, transport, levels, up, down, cols):
    depth, rows, width = tracer.shape
    real = (levels[...] * (1 - land[...])).astype(F32)
    for out, row in ((up, rows - 1), (down, 0)):
        out[0:rows] = surface[...]
        out[rows : 2 * rows] = transport[0]
        out[2 * rows : 3 * rows] = transport[1]
        out[3 * rows : 4 * rows] = real
        for k in range(depth):
            out[4 * rows + k : 4 * rows + k + 1] = tracer[k, row : row + 1]
            at = 4 * rows + depth + k
            out[at : at + 1] = velocity[1, k, row : row + 1]
    lane = lanes_of((8, width))
    first = jnp.zeros((8, width), F32)
    last = jnp.zeros((8, width), F32)
    spot = 0
    for field in range(2):
        for k in range(depth):
            for half in range(0, rows, 8):
                part = tracer[k, half : half + 8] if field == 0 else velocity[0, k, half : half + 8]
                first = jnp.where(lane == spot, part[:, :1], first)
                last = jnp.where(lane == spot, part[:, width - 1 :], last)
                spot += 1
    cols[0:8] = first
    cols[8:16] = last


def edge_kernel(lon, up, south, north, cols, main, extra, eastward, westward):
    rows = up.shape[0] // 8
    width = up.shape[1]
    groups = width // EDGE
    lane = lanes_of((8, width)) // EDGE
    n = 0
    east = west = None
    for field in range(4):
        for block in (south, up, north):
            for half in range(0, rows, 8):
                group = n % groups
                x = block[field * rows + half : field * rows + half + 8]
                to_east = roll(x, EDGE * group - (width - EDGE), 1)
                to_west = roll(x, EDGE * group, 1)
                if group == 0:
                    east, west = to_east, to_west
                else:
                    east = jnp.where(lane == group, to_east, east)
                    west = jnp.where(lane == group, to_west, west)
                n += 1
                if n % groups == 0:
                    at = 8 * (n // groups - 1)
                    eastward[at : at + 8] = east
                    westward[at : at + 8] = west
    at = 8 * (n // groups)
    eastward[at : at + 8] = cols[8:16]
    westward[at : at + 8] = cols[0:8]
    at, size = at + 8, main.shape[0]
    is_first = jnp.full((size, width), lon[0], jnp.int32) == 0
    eastward[at : at + size] = jnp.where(is_first, extra[...], main[...])
    westward[at : at + size] = main[...]
    westward[at + size : at + 2 * size] = extra[...]


def final_kernel(
    n_lon, lon_ref, turn_ref, top_ref, hmix, vmix, tracer, velocity, up, down, south, north, cols, from_west, from_east, main, extra,
    tracer_out, surface_out, transport_out,
    north_own, north_far, seam_own, seam_far, north_rows, primes,
):
    depth, rows, width = tracer.shape
    groups = width // EDGE
    lane8 = lanes_of((8, width))
    half_way = width // 2
    flat = 4 * rows

    def far_tile(n):
        at, group = 8 * (n // groups), n % groups
        east = roll(from_east[at : at + 8], -EDGE * group, 1)
        west = roll(from_west[at : at + 8], (width - EDGE) - EDGE * group, 1)
        return jnp.where(lane8 < half_way, east, west)

    def far_block(field, block):
        first = (field * 3 + block) * (rows // 8)
        return jnp.concatenate([far_tile(first + i) for i in range(rows // 8)], axis=0)

    def shifted(own, far, by):
        lane = lanes_of(own.shape)
        edge = width - 1 if by < 0 else 0
        a, b = roll(own, by, 1), roll(far, by, 1)
        return jnp.where(lane == edge, b, a), jnp.where(lane == edge, a, b)

    at_top = top_ref[0] == 1

    @pl.when(jnp.logical_not(at_top))
    def _():
        north_own[...] = north[0:flat]
        for field in range(4):
            north_far[field * rows : (field + 1) * rows] = far_block(field, 2)
        seam_own[...] = roll(up[3 * rows - 8 : 3 * rows], 1, 0)
        seam_far[...] = roll(far_tile((2 * 3 + 1) * (rows // 8) + rows // 8 - 1), 1, 0)
        north_rows[...] = north[flat : flat + 2 * depth]

    @pl.when(at_top)
    def _():
        turn = turn_ref[0]
        small = jnp.full((8, width), turn, jnp.int32) < half_way
        index = (turn - lane8) & (width - 1)
        less = lane8 <= turn
        back = 7 - rows_of((8, width))

        lon = jnp.full((8, width), lon_ref[0], jnp.int32)
        is_first, is_last = lon == 0, lon == n_lon - 1
        sent = 4 * 3 * rows // groups + 8
        size = main.shape[0]

        def pulled(at):
            mine, other = main[at : at + 8], extra[at : at + 8]
            west = from_west[sent + at : sent + at + 8]
            east = from_east[sent + at : sent + at + 8]
            further = from_east[sent + size + at : sent + size + at + 8]
            g0, g1, g2 = (
                jnp.take_along_axis(x, index, axis=1, mode="promise_in_bounds")
                for x in (
                    jnp.where(is_first, mine, west),
                    jnp.where(is_last, east, jnp.where(is_first, other, mine)),
                    jnp.where(is_last, further, jnp.where(is_first, east, other)),
                )
            )
            own = jnp.where(less, jnp.where(small, g0, g1), jnp.where(small, g1, g2))
            return own, g0, g1, g2

        def turned(x):
            return jnp.take_along_axis(x, back, axis=0, mode="promise_in_bounds")

        for field in range(4):
            own, far = [], []
            for half in range(rows - 8, -8, -8):
                mine, g0, g1, g2 = pulled(field * rows + half)
                low = jnp.where(jnp.logical_and(less, small), g1, g2)
                high = jnp.where(jnp.logical_or(less, small), g0, g1)
                own.append(turned(mine))
                far.append(turned(jnp.where(lane8 < half_way, low, high)))
            own, far = jnp.concatenate(own, axis=0), jnp.concatenate(far, axis=0)
            if field == 1:
                own, far = shifted(-own, -far, -1)
            if field == 2:
                seam_own[...] = -own[:8]
                seam_far[...] = -far[:8]
                own, far = roll(-own, -1, 0), roll(-far, -1, 0)
            north_own[field * rows : (field + 1) * rows] = own
            north_far[field * rows : (field + 1) * rows] = far
        for at in range(0, 2 * depth, 8):
            north_rows[at : at + 8] = pulled(flat + at)[0]

    def window(field):
        at = slice(field * rows, (field + 1) * rows)
        own = jnp.concatenate([south[at], up[at], north_own[at]], axis=0)
        far = jnp.concatenate([far_block(field, 0), far_block(field, 1), north_far[at]], axis=0)
        return own, far

    eta, far_eta = window(0)
    u, far_u = window(1)
    v, far_v = window(2)
    level, far_level = window(3)
    seam, far_seam = seam_own[...], seam_far[...]

    def sea_of(x):
        return (x > 0).astype(F32)

    sea, far_sea = sea_of(level), sea_of(far_level)
    east_sea, east_far_sea = shifted(sea, far_sea, -1)
    east_level, east_far_level = shifted(level, far_level, -1)
    scale = 2.0 * depth
    zmask, far_zmask = sea * east_sea, far_sea * east_far_sea
    zdepth = fb_step * ((level + east_level) / scale)
    far_zdepth = fb_step * ((far_level + east_far_level) / scale)
    mmask, far_mmask = sea * roll(sea, -1, 0), far_sea * roll(far_sea, -1, 0)
    mdepth = fb_step * ((level + roll(level, -1, 0)) / scale)
    far_mdepth = fb_step * ((far_level + roll(far_level, -1, 0)) / scale)
    cut = 2 * rows

    def below(x):
        return roll(x, 1, 0)[cut : cut + 8]

    seam_mask, far_seam_mask = below(mmask), below(far_mmask)
    seam_depth, far_seam_depth = below(mdepth), below(far_mdepth)
    row8 = rows_of((8, width))

    def south_of(x, line):
        moved = roll(x, 1, 0)
        fixed = jnp.where(row8 == 0, line, moved[cut : cut + 8])
        return jnp.concatenate([moved[:cut], fixed, moved[cut + 8 :]], axis=0)

    keep = 1.0 - drag_rate
    for _ in range(SUB):
        west_u, west_far_u = shifted(u, far_u, 1)
        div = (u - west_u) + (v - south_of(v, seam))
        far_div = (far_u - west_far_u) + (far_v - south_of(far_v, far_seam))
        eta = (eta - fb_step * div) * sea
        far_eta = (far_eta - fb_step * far_div) * far_sea
        east, far_east = shifted(eta, far_eta, -1)
        u = (u * keep - zdepth * (east - eta)) * zmask
        far_u = (far_u * keep - far_zdepth * (far_east - far_eta)) * far_zmask
        rise = eta[cut : cut + 8] - below(eta)
        far_rise = far_eta[cut : cut + 8] - below(far_eta)
        seam = (seam * keep - seam_depth * rise) * seam_mask
        far_seam = (far_seam * keep - far_seam_depth * far_rise) * far_seam_mask
        v = (v * keep - mdepth * (roll(eta, -1, 0) - eta)) * mmask
        far_v = (far_v * keep - far_mdepth * (roll(far_eta, -1, 0) - far_eta)) * far_mmask
    mid = slice(rows, 2 * rows)
    surface_out[...] = eta[mid]
    transport_out[0] = u[mid]
    transport_out[1] = v[mid]

    def face(near, beyond, wet_near, wet_beyond, vel_near, vel_beyond, mixing):
        flux = mixing * (beyond - near) - 0.25 * (vel_near + vel_beyond) * (near + beyond)
        return jnp.where(jnp.logical_and(wet_near, wet_beyond), flux, 0.0)

    level_row = rows_of((depth, width)).astype(F32)
    mix_rows = jnp.zeros((depth, width), F32)
    for k in range(depth):
        mix_rows = jnp.where(level_row == k, hmix[k], mix_rows)
    top, bottom = level[2 * rows - 1 : 2 * rows], level[rows : rows + 1]
    flux_top = face(
        up[flat : flat + depth],
        north_rows[0:depth],
        level_row < top,
        level_row < level[2 * rows : 2 * rows + 1],
        up[flat + depth : flat + 2 * depth],
        north_rows[depth : 2 * depth],
        mix_rows,
    )
    flux_bottom = face(
        south[flat : flat + depth],
        down[flat : flat + depth],
        level_row < level[rows - 1 : rows],
        level_row < bottom,
        south[flat + depth : flat + 2 * depth],
        down[flat + depth : flat + 2 * depth],
        mix_rows,
    )
    parts = rows // 8
    level_lane = ((lane8 & (parts * depth - 1)) // parts).astype(F32)
    mix_lanes = jnp.zeros((8, width), F32)
    for k in range(depth):
        mix_lanes = jnp.where(level_lane == k, hmix[k], mix_lanes)
    here, far_here = level[mid], far_level[mid]

    def column(x, at):
        packed = jnp.broadcast_to(x[:8, at : at + 1], (8, width))
        for i in range(1, parts):
            packed = jnp.where(lane8 % parts == i, x[8 * i : 8 * i + 8, at : at + 1], packed)
        return packed

    def side(near, beyond, level_near, level_beyond):
        return face(
            near,
            beyond,
            level_lane < level_near,
            level_lane < level_beyond,
            roll(near, -half_way, 1),
            roll(beyond, -half_way, 1),
            mix_lanes,
        )

    spot = 8 * (4 * 3 * parts // groups)
    flux_right = side(
        cols[8:16], from_east[spot : spot + 8], column(here, width - 1), column(far_here, 0)
    )
    flux_left = side(
        from_west[spot : spot + 8], cols[0:8], column(far_here, width - 1), column(here, 0)
    )

    lane = lanes_of((rows, width))
    row = rows_of((rows, width))
    here_east = roll(here, -1, 1)
    here_north = roll(here, -1, 0)

    def spread(x, k):
        return jnp.concatenate(
            [jnp.broadcast_to(x[:, parts * k + i : parts * k + i + 1], (8, width)) for i in range(parts)],
            axis=0,
        )

    sweep = prime = link = None
    for k in range(depth):
        field, zonal, merid = tracer[k], velocity[0, k], velocity[1, k]
        wet = here > k
        mixing = hmix[k]
        east_flux = face(
            field, roll(field, -1, 1), wet, here_east > k, zonal, roll(zonal, -1, 1), mixing
        )
        east_flux = jnp.where(lane == width - 1, spread(flux_right, k), east_flux)
        west_flux = jnp.where(lane == 0, spread(flux_left, k), roll(east_flux, 1, 1))
        north_flux = face(
            field, roll(field, -1, 0), wet, here_north > k, merid, roll(merid, -1, 0), mixing
        )
        north_flux = jnp.where(row == rows - 1, flux_top[k : k + 1], north_flux)
        south_flux = jnp.where(row == 0, flux_bottom[k : k + 1], roll(north_flux, 1, 0))
        stepped = jnp.where(
            wet, field + ((east_flux - west_flux) + (north_flux - south_flux)), 0.0
        )
        diagonal = jnp.ones_like(stepped)
        if k > 0:
            diagonal = diagonal + link
        if k < depth - 1:
            next_link = jnp.where(here > k + 1, vmix[k], 0.0)
            diagonal = diagonal + next_link
        if k > 0:
            diagonal = diagonal + link * prime
            stepped = stepped + link * sweep
        inverse = 1.0 / diagonal
        sweep = stepped * inverse
        tracer_out[k] = sweep
        if k < depth - 1:
            prime = -next_link * inverse
            primes[k] = prime
            link = next_link
    solved = sweep
    for k in range(depth - 2, -1, -1):
        solved = tracer_out[k] - primes[k] * solved
        tracer_out[k] = solved


def shards(
    tracer, velocity, surface, transport, horiz_mixing, vert_mixing, levels, land_tiles, fold_pair,
    *, n_lon, n_lat, interpret,
):
    depth, rows, width = tracer.shape
    smem = pl.BlockSpec(memory_space=pltpu.SMEM)
    vmem = pl.BlockSpec(memory_space=pltpu.VMEM)
    call = functools.partial(pl.pallas_call, interpret=interpret)

    def like(*shape):
        return jax.ShapeDtypeStruct(shape, F32)

    stack = 4 * rows + 2 * depth
    up, down, cols = call(
        pack_kernel,
        out_shape=(like(stack, width), like(stack, width), like(16, width)),
        in_specs=[vmem] * 6,
        out_specs=(vmem,) * 3,
        name="pack",
    )(land_tiles, tracer, velocity, surface, transport, levels)

    south = lax.ppermute(up, "lat", [(i, i + 1) for i in range(n_lat - 1)])
    north = lax.ppermute(down, "lat", [(i + 1, i) for i in range(n_lat - 1)])

    lon = lax.axis_index("lon")
    pivot = (fold_pair[0] + width * lon) % (width * n_lon)
    turn = pivot % width
    tile = (pivot // width - (turn < width // 2).astype(jnp.int32)) % n_lon

    def fetch(x, shift):
        routes = [(shift + 1, 0)] + [(shift - t, t) for t in range(1, n_lon - 1)]
        pairs = [(s % n_lon * n_lat + n_lat - 1, t * n_lat + n_lat - 1) for s, t in routes]
        return lax.ppermute(x, ("lon", "lat"), pairs)

    def branch(shift):
        def both(x):
            later = fetch(x, (shift - 1) % n_lon)
            return later, fetch(x, shift)

        return both

    extra, main = lax.switch(tile, [branch(shift) for shift in range(n_lon)], up)

    at_top = (lax.axis_index("lat") == n_lat - 1).astype(jnp.int32)
    lon, turn, at_top = (x.reshape(1) for x in (lon, turn, at_top))
    edge_rows = 4 * 3 * rows * EDGE // width + 8
    eastward, westward = call(
        edge_kernel,
        out_shape=(like(edge_rows + stack, width), like(edge_rows + 2 * stack, width)),
        in_specs=[smem] + [vmem] * 6,
        out_specs=(vmem,) * 2,
        name="edge",
    )(lon, up, south, north, cols, main, extra)
    from_west = lax.ppermute(eastward, "lon", [(i, (i + 1) % n_lon) for i in range(n_lon)])
    from_east = lax.ppermute(westward, "lon", [((i + 1) % n_lon, i) for i in range(n_lon)])

    return call(
        functools.partial(final_kernel, n_lon),
        out_shape=(like(depth, rows, width), like(rows, width), like(2, rows, width)),
        in_specs=[smem] * 5 + [vmem] * 11,
        out_specs=(vmem,) * 3,
        scratch_shapes=[
            pltpu.VMEM((4 * rows, width), F32),
            pltpu.VMEM((4 * rows, width), F32),
            pltpu.VMEM((8, width), F32),
            pltpu.VMEM((8, width), F32),
            pltpu.VMEM((2 * depth, width), F32),
            pltpu.VMEM((depth, rows, width), F32),
        ],
        name="final",
    )(
        lon, turn, at_top, horiz_mixing, vert_mixing, tracer, velocity, up, down, south, north, cols,
        from_west, from_east, main, extra,
    )


def solution(mesh, interpret=False):
    def step(*args):
        return shards(*args, n_lon=mesh.shape["lon"], n_lat=mesh.shape["lat"], interpret=interpret)

    return jax.shard_map(
        step,
        mesh=mesh,
        in_specs=(
            P("member", "lat", "lon"),
            P(None, "member", "lat", "lon"),
            P(("member", "lat"), "lon"),
            P("member", "lat", "lon"),
            P("member"),
            P("member"),
            P("lat", "lon"),
            P("lat", "lon"),
            P("lon"),
        ),
        out_specs=(
            P("member", "lat", "lon"),
            P(("member", "lat"), "lon"),
            P("member", "lat", "lon"),
        ),
        check_vma=False,
    )
```

```python
import functools

import jax
import jax.numpy as jnp
from jax import lax
from jax.experimental import pallas as pl
from jax.experimental.pallas import tpu as pltpu
from jax.sharding import PartitionSpec as P


SUB = 12
fb_step = 0.6
drag_rate = 0.02
EDGE = 16
F32 = jnp.float32


def lanes_of(shape):
    return lax.broadcasted_iota(jnp.int32, shape, 1)


def rows_of(shape):
    return lax.broadcasted_iota(jnp.int32, shape, 0)


def roll(x, shift, axis):
    return pltpu.roll(x, shift % x.shape[axis], axis)


def pack_kernel(land, tracer, velocity, surface, transport, levels, up, down, cols):
    depth, rows, width = tracer.shape
    real = (levels[...] * (1 - land[...])).astype(F32)
    for out, row in ((up, rows - 1), (down, 0)):
        out[0:rows] = surface[...]
        out[rows : 2 * rows] = transport[0]
        out[2 * rows : 3 * rows] = transport[1]
        out[3 * rows : 4 * rows] = real
        for k in range(depth):
            out[4 * rows + k : 4 * rows + k + 1] = tracer[k, row : row + 1]
            at = 4 * rows + depth + k
            out[at : at + 1] = velocity[1, k, row : row + 1]
    lane = lanes_of((8, width))
    first = jnp.zeros((8, width), F32)
    last = jnp.zeros((8, width), F32)
    spot = 0
    for field in range(2):
        for k in range(depth):
            for half in range(0, rows, 8):
                part = tracer[k, half : half + 8] if field == 0 else velocity[0, k, half : half + 8]
                first = jnp.where(lane == spot, part[:, :1], first)
                last = jnp.where(lane == spot, part[:, width - 1 :], last)
                spot += 1
    cols[0:8] = first
    cols[8:16] = last


def edge_kernel(lon, up, south, north, cols, main, extra, eastward, westward):
    rows = up.shape[0] // 8
    width = up.shape[1]
    groups = width // EDGE
    lane = lanes_of((8, width)) // EDGE
    n = 0
    east = west = None
    for field in range(4):
        for block in (south, up, north):
            for half in range(0, rows, 8):
                group = n % groups
                x = block[field * rows + half : field * rows + half + 8]
                to_east = roll(x, EDGE * group - (width - EDGE), 1)
                to_west = roll(x, EDGE * group, 1)
                if group == 0:
                    east, west = to_east, to_west
                else:
                    east = jnp.where(lane == group, to_east, east)
                    west = jnp.where(lane == group, to_west, west)
                n += 1
                if n % groups == 0:
                    at = 8 * (n // groups - 1)
                    eastward[at : at + 8] = east
                    westward[at : at + 8] = west
    at = 8 * (n // groups)
    eastward[at : at + 8] = cols[8:16]
    westward[at : at + 8] = cols[0:8]
    at, size = at + 8, main.shape[0]
    is_first = jnp.full((size, width), lon[0], jnp.int32) == 0
    eastward[at : at + size] = jnp.where(is_first, extra[...], main[...])
    westward[at : at + size] = main[...]
    westward[at + size : at + 2 * size] = extra[...]


def final_kernel(
    n_lon, lon_ref, turn_ref, top_ref, hmix, vmix, tracer, velocity, up, down, south, north, cols, from_west, from_east, main, extra,
    tracer_out, surface_out, transport_out,
    north_own, north_far, seam_own, seam_far, north_rows, primes,
):
    depth, rows, width = tracer.shape
    groups = width // EDGE
    lane8 = lanes_of((8, width))
    half_way = width // 2
    flat = 4 * rows

    def far_tile(n):
        at, group = 8 * (n // groups), n % groups
        east = roll(from_east[at : at + 8], -EDGE * group, 1)
        west = roll(from_west[at : at + 8], (width - EDGE) - EDGE * group, 1)
        return jnp.where(lane8 < half_way, east, west)

    def far_block(field, block):
        first = (field * 3 + block) * (rows // 8)
        return jnp.concatenate([far_tile(first + i) for i in range(rows // 8)], axis=0)

    def shifted(own, far, by):
        lane = lanes_of(own.shape)
        edge = width - 1 if by < 0 else 0
        a, b = roll(own, by, 1), roll(far, by, 1)
        return jnp.where(lane == edge, b, a), jnp.where(lane == edge, a, b)

    at_top = top_ref[0] == 1

    @pl.when(jnp.logical_not(at_top))
    def _():
        north_own[...] = north[0:flat]
        for field in range(4):
            north_far[field * rows : (field + 1) * rows] = far_block(field, 2)
        seam_own[...] = roll(up[3 * rows - 8 : 3 * rows], 1, 0)
        seam_far[...] = roll(far_tile((2 * 3 + 1) * (rows // 8) + rows // 8 - 1), 1, 0)
        north_rows[...] = north[flat : flat + 2 * depth]

    @pl.when(at_top)
    def _():
        turn = turn_ref[0]
        small = jnp.full((8, width), turn, jnp.int32) < half_way
        index = (turn - lane8) & (width - 1)
        less = lane8 <= turn
        back = 7 - rows_of((8, width))

        lon = jnp.full((8, width), lon_ref[0], jnp.int32)
        is_first, is_last = lon == 0, lon == n_lon - 1
        sent = 4 * 3 * rows // groups + 8
        size = main.shape[0]

        def pulled(at):
            mine, other = main[at : at + 8], extra[at : at + 8]
            west = from_west[sent + at : sent + at + 8]
            east = from_east[sent + at : sent + at + 8]
            further = from_east[sent + size + at : sent + size + at + 8]
            g0, g1, g2 = (
                jnp.take_along_axis(x, index, axis=1, mode="promise_in_bounds")
                for x in (
                    jnp.where(is_first, mine, west),
                    jnp.where(is_last, east, jnp.where(is_first, other, mine)),
                    jnp.where(is_last, further, jnp.where(is_first, east, other)),
                )
            )
            own = jnp.where(less, jnp.where(small, g0, g1), jnp.where(small, g1, g2))
            return own, g0, g1, g2

        def turned(x):
            return jnp.take_along_axis(x, back, axis=0, mode="promise_in_bounds")

        for field in range(4):
            own, far = [], []
            for half in range(rows - 8, -8, -8):
                mine, g0, g1, g2 = pulled(field * rows + half)
                low = jnp.where(jnp.logical_and(less, small), g1, g2)
                high = jnp.where(jnp.logical_or(less, small), g0, g1)
                own.append(turned(mine))
                far.append(turned(jnp.where(lane8 < half_way, low, high)))
            own, far = jnp.concatenate(own, axis=0), jnp.concatenate(far, axis=0)
            if field == 1:
                own, far = shifted(-own, -far, -1)
            if field == 2:
                seam_own[...] = -own[:8]
                seam_far[...] = -far[:8]
                own, far = roll(-own, -1, 0), roll(-far, -1, 0)
            north_own[field * rows : (field + 1) * rows] = own
            north_far[field * rows : (field + 1) * rows] = far
        for at in range(0, 2 * depth, 8):
            north_rows[at : at + 8] = pulled(flat + at)[0]

    def window(field):
        at = slice(field * rows, (field + 1) * rows)
        own = jnp.concatenate([south[at], up[at], north_own[at]], axis=0)
        far = jnp.concatenate([far_block(field, 0), far_block(field, 1), north_far[at]], axis=0)
        return own, far

    eta, far_eta = window(0)
    u, far_u = window(1)
    v, far_v = window(2)
    level, far_level = window(3)
    seam, far_seam = seam_own[...], seam_far[...]

    def sea_of(x):
        return (x > 0).astype(F32)

    sea, far_sea = sea_of(level), sea_of(far_level)
    east_sea, east_far_sea = shifted(sea, far_sea, -1)
    east_level, east_far_level = shifted(level, far_level, -1)
    scale = 2.0 * depth
    zmask, far_zmask = sea * east_sea, far_sea * east_far_sea
    zdepth = fb_step * ((level + east_level) / scale)
    far_zdepth = fb_step * ((far_level + east_far_level) / scale)
    mmask, far_mmask = sea * roll(sea, -1, 0), far_sea * roll(far_sea, -1, 0)
    mdepth = fb_step * ((level + roll(level, -1, 0)) / scale)
    far_mdepth = fb_step * ((far_level + roll(far_level, -1, 0)) / scale)
    cut = 2 * rows

    def below(x):
        return roll(x, 1, 0)[cut : cut + 8]

    seam_mask, far_seam_mask = below(mmask), below(far_mmask)
    seam_depth, far_seam_depth = below(mdepth), below(far_mdepth)
    row8 = rows_of((8, width))

    def south_of(x, line):
        moved = roll(x, 1, 0)
        fixed = jnp.where(row8 == 0, line, moved[cut : cut + 8])
        return jnp.concatenate([moved[:cut], fixed, moved[cut + 8 :]], axis=0)

    keep = 1.0 - drag_rate
    for _ in range(SUB):
        west_u, west_far_u = shifted(u, far_u, 1)
        div = (u - west_u) + (v - south_of(v, seam))
        far_div = (far_u - west_far_u) + (far_v - south_of(far_v, far_seam))
        eta = (eta - fb_step * div) * sea
        far_eta = (far_eta - fb_step * far_div) * far_sea
        east, far_east = shifted(eta, far_eta, -1)
        u = (u * keep - zdepth * (east - eta)) * zmask
        far_u = (far_u * keep - far_zdepth * (far_east - far_eta)) * far_zmask
        rise = eta[cut : cut + 8] - below(eta)
        far_rise = far_eta[cut : cut + 8] - below(far_eta)
        seam = (seam * keep - seam_depth * rise) * seam_mask
        far_seam = (far_seam * keep - far_seam_depth * far_rise) * far_seam_mask
        v = (v * keep - mdepth * (roll(eta, -1, 0) - eta)) * mmask
        far_v = (far_v * keep - far_mdepth * (roll(far_eta, -1, 0) - far_eta)) * far_mmask
    mid = slice(rows, 2 * rows)
    surface_out[...] = eta[mid]
    transport_out[0] = u[mid]
    transport_out[1] = v[mid]

    def face(near, beyond, wet_near, wet_beyond, vel_near, vel_beyond, mixing):
        flux = mixing * (beyond - near) - 0.25 * (vel_near + vel_beyond) * (near + beyond)
        return jnp.where(jnp.logical_and(wet_near, wet_beyond), flux, 0.0)

    level_row = rows_of((depth, width)).astype(F32)
    mix_rows = jnp.zeros((depth, width), F32)
    for k in range(depth):
        mix_rows = jnp.where(level_row == k, hmix[k], mix_rows)
    top, bottom = level[2 * rows - 1 : 2 * rows], level[rows : rows + 1]
    flux_top = face(
        up[flat : flat + depth],
        north_rows[0:depth],
        level_row < top,
        level_row < level[2 * rows : 2 * rows + 1],
        up[flat + depth : flat + 2 * depth],
        north_rows[depth : 2 * depth],
        mix_rows,
    )
    flux_bottom = face(
        south[flat : flat + depth],
        down[flat : flat + depth],
        level_row < level[rows - 1 : rows],
        level_row < bottom,
        south[flat + depth : flat + 2 * depth],
        down[flat + depth : flat + 2 * depth],
        mix_rows,
    )
    parts = rows // 8
    level_lane = ((lane8 & (parts * depth - 1)) // parts).astype(F32)
    mix_lanes = jnp.zeros((8, width), F32)
    for k in range(depth):
        mix_lanes = jnp.where(level_lane == k, hmix[k], mix_lanes)
    here, far_here = level[mid], far_level[mid]

    def column(x, at):
        packed = jnp.broadcast_to(x[:8, at : at + 1], (8, width))
        for i in range(1, parts):
            packed = jnp.where(lane8 % parts == i, x[8 * i : 8 * i + 8, at : at + 1], packed)
        return packed

    def side(near, beyond, level_near, level_beyond):
        return face(
            near,
            beyond,
            level_lane < level_near,
            level_lane < level_beyond,
            roll(near, -half_way, 1),
            roll(beyond, -half_way, 1),
            mix_lanes,
        )

    spot = 8 * (4 * 3 * parts // groups)
    flux_right = side(
        cols[8:16], from_east[spot : spot + 8], column(here, width - 1), column(far_here, 0)
    )
    flux_left = side(
        from_west[spot : spot + 8], cols[0:8], column(far_here, width - 1), column(here, 0)
    )

    lane = lanes_of((rows, width))
    row = rows_of((rows, width))
    here_east = roll(here, -1, 1)
    here_north = roll(here, -1, 0)

    def spread(x, k):
        return jnp.concatenate(
            [jnp.broadcast_to(x[:, parts * k + i : parts * k + i + 1], (8, width)) for i in range(parts)],
            axis=0,
        )

    sweep = prime = link = None
    for k in range(depth):
        field, zonal, merid = tracer[k], velocity[0, k], velocity[1, k]
        wet = here > k
        mixing = hmix[k]
        east_flux = face(
            field, roll(field, -1, 1), wet, here_east > k, zonal, roll(zonal, -1, 1), mixing
        )
        east_flux = jnp.where(lane == width - 1, spread(flux_right, k), east_flux)
        west_flux = jnp.where(lane == 0, spread(flux_left, k), roll(east_flux, 1, 1))
        north_flux = face(
            field, roll(field, -1, 0), wet, here_north > k, merid, roll(merid, -1, 0), mixing
        )
        north_flux = jnp.where(row == rows - 1, flux_top[k : k + 1], north_flux)
        south_flux = jnp.where(row == 0, flux_bottom[k : k + 1], roll(north_flux, 1, 0))
        stepped = jnp.where(
            wet, field + ((east_flux - west_flux) + (north_flux - south_flux)), 0.0
        )
        diagonal = jnp.ones_like(stepped)
        if k > 0:
            diagonal = diagonal + link
        if k < depth - 1:
            next_link = jnp.where(here > k + 1, vmix[k], 0.0)
            diagonal = diagonal + next_link
        if k > 0:
            diagonal = diagonal + link * prime
            stepped = stepped + link * sweep
        inverse = 1.0 / diagonal
        sweep = stepped * inverse
        tracer_out[k] = sweep
        if k < depth - 1:
            prime = -next_link * inverse
            primes[k] = prime
            link = next_link
    solved = sweep
    for k in range(depth - 2, -1, -1):
        solved = tracer_out[k] - primes[k] * solved
        tracer_out[k] = solved


def shards(
    tracer, velocity, surface, transport, horiz_mixing, vert_mixing, levels, land_tiles, fold_pair,
    *, n_lon, n_lat, interpret,
):
    depth, rows, width = tracer.shape
    smem = pl.BlockSpec(memory_space=pltpu.SMEM)
    vmem = pl.BlockSpec(memory_space=pltpu.VMEM)
    call = functools.partial(pl.pallas_call, interpret=interpret)

    def like(*shape):
        return jax.ShapeDtypeStruct(shape, F32)

    def on_chip(*shape):
        return like(*shape) if interpret else pltpu.VMEM(shape, F32)

    def held(x):
        return x if interpret else pltpu.with_memory_space_constraint(x, pltpu.VMEM)

    stack = 4 * rows + 2 * depth
    up, down, cols = call(
        pack_kernel,
        out_shape=(on_chip(stack, width), on_chip(stack, width), on_chip(16, width)),
        in_specs=[vmem] * 6,
        out_specs=(vmem,) * 3,
        name="pack",
    )(land_tiles, tracer, velocity, surface, transport, levels)

    south = lax.ppermute(up, "lat", [(i, i + 1) for i in range(n_lat - 1)])
    north = lax.ppermute(down, "lat", [(i + 1, i) for i in range(n_lat - 1)])

    lon = lax.axis_index("lon")
    pivot = (fold_pair[0] + width * lon) % (width * n_lon)
    turn = pivot % width
    tile = (pivot // width - (turn < width // 2).astype(jnp.int32)) % n_lon

    def fetch(x, shift):
        routes = [(shift + 1, 0)] + [(shift - t, t) for t in range(1, n_lon - 1)]
        pairs = [(s % n_lon * n_lat + n_lat - 1, t * n_lat + n_lat - 1) for s, t in routes]
        return lax.ppermute(x, ("lon", "lat"), pairs)

    def branch(shift):
        def both(x):
            later = fetch(x, (shift - 1) % n_lon)
            return later, fetch(x, shift)

        return both

    extra, main = lax.switch(tile, [branch(shift) for shift in range(n_lon)], up)

    at_top = (lax.axis_index("lat") == n_lat - 1).astype(jnp.int32)
    lon, turn, at_top = (x.reshape(1) for x in (lon, turn, at_top))
    edge_rows = 4 * 3 * rows * EDGE // width + 8
    eastward, westward = call(
        edge_kernel,
        out_shape=(on_chip(edge_rows + stack, width), on_chip(edge_rows + 2 * stack, width)),
        in_specs=[smem] + [vmem] * 6,
        out_specs=(vmem,) * 2,
        name="edge",
    )(lon, *map(held, (up, south, north, cols, main, extra)))
    from_west = lax.ppermute(eastward, "lon", [(i, (i + 1) % n_lon) for i in range(n_lon)])
    from_east = lax.ppermute(westward, "lon", [((i + 1) % n_lon, i) for i in range(n_lon)])

    return call(
        functools.partial(final_kernel, n_lon),
        out_shape=(like(depth, rows, width), like(rows, width), like(2, rows, width)),
        in_specs=[smem] * 5 + [vmem] * 11,
        out_specs=(vmem,) * 3,
        scratch_shapes=[
            pltpu.VMEM((4 * rows, width), F32),
            pltpu.VMEM((4 * rows, width), F32),
            pltpu.VMEM((8, width), F32),
            pltpu.VMEM((8, width), F32),
            pltpu.VMEM((2 * depth, width), F32),
            pltpu.VMEM((depth, rows, width), F32),
        ],
        name="final",
    )(
        lon, turn, at_top, horiz_mixing, vert_mixing, tracer, velocity,
        *map(held, (up, down, south, north, cols, from_west, from_east, main, extra)),
    )


def solution(mesh, interpret=False):
    def step(*args):
        return shards(*args, n_lon=mesh.shape["lon"], n_lat=mesh.shape["lat"], interpret=interpret)

    return jax.shard_map(
        step,
        mesh=mesh,
        in_specs=(
            P("member", "lat", "lon"),
            P(None, "member", "lat", "lon"),
            P(("member", "lat"), "lon"),
            P("member", "lat", "lon"),
            P("member"),
            P("member"),
            P("lat", "lon"),
            P("lat", "lon"),
            P("lon"),
        ),
        out_specs=(
            P("member", "lat", "lon"),
            P(("member", "lat"), "lon"),
            P("member", "lat", "lon"),
        ),
        check_vma=False,
    )
```

```python
import functools

import jax
import jax.numpy as jnp
from jax import lax
from jax.experimental import pallas as pl
from jax.experimental.pallas import tpu as pltpu
from jax.sharding import PartitionSpec as P


SUB = 12
fb_step = 0.6
drag_rate = 0.02
EDGE = 16
F32 = jnp.float32


def lanes_of(shape):
    return lax.broadcasted_iota(jnp.int32, shape, 1)


def rows_of(shape):
    return lax.broadcasted_iota(jnp.int32, shape, 0)


def roll(x, shift, axis):
    return pltpu.roll(x, shift % x.shape[axis], axis)


def pack_kernel(land, tracer, velocity, surface, transport, levels, up, down, cols):
    depth, rows, width = tracer.shape
    real = (levels[...] * (1 - land[...])).astype(F32)
    for out, row in ((up, rows - 1), (down, 0)):
        out[0:rows] = surface[...]
        out[rows : 2 * rows] = transport[0]
        out[2 * rows : 3 * rows] = transport[1]
        out[3 * rows : 4 * rows] = real
        for k in range(depth):
            out[4 * rows + k : 4 * rows + k + 1] = tracer[k, row : row + 1]
            at = 4 * rows + depth + k
            out[at : at + 1] = velocity[1, k, row : row + 1]
    lane = lanes_of((8, width))
    first = jnp.zeros((8, width), F32)
    last = jnp.zeros((8, width), F32)
    spot = 0
    for field in range(2):
        for k in range(depth):
            for half in range(0, rows, 8):
                part = tracer[k, half : half + 8] if field == 0 else velocity[0, k, half : half + 8]
                first = jnp.where(lane == spot, part[:, :1], first)
                last = jnp.where(lane == spot, part[:, width - 1 :], last)
                spot += 1
    cols[0:8] = first
    cols[8:16] = last


def edge_kernel(lon, up, south, north, cols, main, extra, eastward, westward):
    rows = up.shape[0] // 8
    width = up.shape[1]
    groups = width // EDGE
    lane = lanes_of((8, width)) // EDGE
    n = 0
    east = west = None
    for field in range(4):
        for block in (south, up, north):
            for half in range(0, rows, 8):
                group = n % groups
                x = block[field * rows + half : field * rows + half + 8]
                to_east = roll(x, EDGE * group - (width - EDGE), 1)
                to_west = roll(x, EDGE * group, 1)
                if group == 0:
                    east, west = to_east, to_west
                else:
                    east = jnp.where(lane == group, to_east, east)
                    west = jnp.where(lane == group, to_west, west)
                n += 1
                if n % groups == 0:
                    at = 8 * (n // groups - 1)
                    eastward[at : at + 8] = east
                    westward[at : at + 8] = west
    at = 8 * (n // groups)
    eastward[at : at + 8] = cols[8:16]
    westward[at : at + 8] = cols[0:8]
    at, size = at + 8, main.shape[0]
    is_first = jnp.full((size, width), lon[0], jnp.int32) == 0
    eastward[at : at + size] = jnp.where(is_first, extra[...], main[...])
    westward[at : at + size] = main[...]
    westward[at + size : at + 2 * size] = extra[...]


def face(near, beyond, wet_near, wet_beyond, vel_near, vel_beyond, mixing):
    flux = mixing * (beyond - near) - 0.25 * (vel_near + vel_beyond) * (near + beyond)
    return jnp.where(jnp.logical_and(wet_near, wet_beyond), flux, 0.0)


def interior_kernel(hmix, vmix, tracer, velocity, up, inner, inverses, carries, primes):
    depth, rows, width = tracer.shape
    here = up[3 * rows : 4 * rows]
    lane = lanes_of((rows, width))
    row = rows_of((rows, width))
    here_east = roll(here, -1, 1)
    here_north = roll(here, -1, 0)
    prime = link = None
    for k in range(depth):
        field, zonal, merid = tracer[k], velocity[0, k], velocity[1, k]
        wet = here > k
        mixing = hmix[k]
        east_flux = face(
            field, roll(field, -1, 1), wet, here_east > k, zonal, roll(zonal, -1, 1), mixing
        )
        east_flux = jnp.where(lane == width - 1, 0.0, east_flux)
        north_flux = face(
            field, roll(field, -1, 0), wet, here_north > k, merid, roll(merid, -1, 0), mixing
        )
        north_flux = jnp.where(row == rows - 1, 0.0, north_flux)
        inner[k] = field + (
            (east_flux - roll(east_flux, 1, 1)) + (north_flux - roll(north_flux, 1, 0))
        )
        diagonal = jnp.ones_like(field)
        if k > 0:
            diagonal = diagonal + link
        if k < depth - 1:
            next_link = jnp.where(here > k + 1, vmix[k], 0.0)
            diagonal = diagonal + next_link
        if k > 0:
            diagonal = diagonal + link * prime
        inverse = 1.0 / diagonal
        inverses[k] = inverse
        if k > 0:
            carries[k - 1] = link * inverse
        if k < depth - 1:
            prime = -next_link * inverse
            primes[k] = prime
            link = next_link


def final_kernel(
    n_lon, lon_ref, turn_ref, top_ref, hmix, inner, inverses, carries, primes, up, down, south, north, cols, from_west, from_east, main, extra,
    tracer_out, surface_out, transport_out,
    north_own, north_far, seam_own, seam_far, north_rows,
):
    depth, rows, width = inner.shape
    groups = width // EDGE
    lane8 = lanes_of((8, width))
    half_way = width // 2
    flat = 4 * rows

    def far_tile(n):
        at, group = 8 * (n // groups), n % groups
        east = roll(from_east[at : at + 8], -EDGE * group, 1)
        west = roll(from_west[at : at + 8], (width - EDGE) - EDGE * group, 1)
        return jnp.where(lane8 < half_way, east, west)

    def far_block(field, block):
        first = (field * 3 + block) * (rows // 8)
        return jnp.concatenate([far_tile(first + i) for i in range(rows // 8)], axis=0)

    def shifted(own, far, by):
        lane = lanes_of(own.shape)
        edge = width - 1 if by < 0 else 0
        a, b = roll(own, by, 1), roll(far, by, 1)
        return jnp.where(lane == edge, b, a), jnp.where(lane == edge, a, b)

    at_top = top_ref[0] == 1

    @pl.when(jnp.logical_not(at_top))
    def _():
        north_own[...] = north[0:flat]
        for field in range(4):
            north_far[field * rows : (field + 1) * rows] = far_block(field, 2)
        seam_own[...] = roll(up[3 * rows - 8 : 3 * rows], 1, 0)
        seam_far[...] = roll(far_tile((2 * 3 + 1) * (rows // 8) + rows // 8 - 1), 1, 0)
        north_rows[...] = north[flat : flat + 2 * depth]

    @pl.when(at_top)
    def _():
        turn = turn_ref[0]
        small = jnp.full((8, width), turn, jnp.int32) < half_way
        index = (turn - lane8) & (width - 1)
        less = lane8 <= turn
        back = 7 - rows_of((8, width))

        lon = jnp.full((8, width), lon_ref[0], jnp.int32)
        is_first, is_last = lon == 0, lon == n_lon - 1
        sent = 4 * 3 * rows // groups + 8
        size = main.shape[0]

        def pulled(at):
            mine, other = main[at : at + 8], extra[at : at + 8]
            west = from_west[sent + at : sent + at + 8]
            east = from_east[sent + at : sent + at + 8]
            further = from_east[sent + size + at : sent + size + at + 8]
            g0, g1, g2 = (
                jnp.take_along_axis(x, index, axis=1, mode="promise_in_bounds")
                for x in (
                    jnp.where(is_first, mine, west),
                    jnp.where(is_last, east, jnp.where(is_first, other, mine)),
                    jnp.where(is_last, further, jnp.where(is_first, east, other)),
                )
            )
            own = jnp.where(less, jnp.where(small, g0, g1), jnp.where(small, g1, g2))
            return own, g0, g1, g2

        def turned(x):
            return jnp.take_along_axis(x, back, axis=0, mode="promise_in_bounds")

        for field in range(4):
            own, far = [], []
            for half in range(rows - 8, -8, -8):
                mine, g0, g1, g2 = pulled(field * rows + half)
                low = jnp.where(jnp.logical_and(less, small), g1, g2)
                high = jnp.where(jnp.logical_or(less, small), g0, g1)
                own.append(turned(mine))
                far.append(turned(jnp.where(lane8 < half_way, low, high)))
            own, far = jnp.concatenate(own, axis=0), jnp.concatenate(far, axis=0)
            if field == 1:
                own, far = shifted(-own, -far, -1)
            if field == 2:
                seam_own[...] = -own[:8]
                seam_far[...] = -far[:8]
                own, far = roll(-own, -1, 0), roll(-far, -1, 0)
            north_own[field * rows : (field + 1) * rows] = own
            north_far[field * rows : (field + 1) * rows] = far
        for at in range(0, 2 * depth, 8):
            north_rows[at : at + 8] = pulled(flat + at)[0]

    def window(field):
        at = slice(field * rows, (field + 1) * rows)
        own = jnp.concatenate([south[at], up[at], north_own[at]], axis=0)
        far = jnp.concatenate([far_block(field, 0), far_block(field, 1), north_far[at]], axis=0)
        return own, far

    eta, far_eta = window(0)
    u, far_u = window(1)
    v, far_v = window(2)
    level, far_level = window(3)
    seam, far_seam = seam_own[...], seam_far[...]

    def sea_of(x):
        return (x > 0).astype(F32)

    sea, far_sea = sea_of(level), sea_of(far_level)
    east_sea, east_far_sea = shifted(sea, far_sea, -1)
    east_level, east_far_level = shifted(level, far_level, -1)
    scale = 2.0 * depth
    zmask, far_zmask = sea * east_sea, far_sea * east_far_sea
    zdepth = fb_step * ((level + east_level) / scale)
    far_zdepth = fb_step * ((far_level + east_far_level) / scale)
    mmask, far_mmask = sea * roll(sea, -1, 0), far_sea * roll(far_sea, -1, 0)
    mdepth = fb_step * ((level + roll(level, -1, 0)) / scale)
    far_mdepth = fb_step * ((far_level + roll(far_level, -1, 0)) / scale)
    cut = 2 * rows

    def below(x):
        return roll(x, 1, 0)[cut : cut + 8]

    seam_mask, far_seam_mask = below(mmask), below(far_mmask)
    seam_depth, far_seam_depth = below(mdepth), below(far_mdepth)
    row8 = rows_of((8, width))

    def south_of(x, line):
        moved = roll(x, 1, 0)
        fixed = jnp.where(row8 == 0, line, moved[cut : cut + 8])
        return jnp.concatenate([moved[:cut], fixed, moved[cut + 8 :]], axis=0)

    keep = 1.0 - drag_rate
    for _ in range(SUB):
        west_u, west_far_u = shifted(u, far_u, 1)
        div = (u - west_u) + (v - south_of(v, seam))
        far_div = (far_u - west_far_u) + (far_v - south_of(far_v, far_seam))
        eta = (eta - fb_step * div) * sea
        far_eta = (far_eta - fb_step * far_div) * far_sea
        east, far_east = shifted(eta, far_eta, -1)
        u = (u * keep - zdepth * (east - eta)) * zmask
        far_u = (far_u * keep - far_zdepth * (far_east - far_eta)) * far_zmask
        rise = eta[cut : cut + 8] - below(eta)
        far_rise = far_eta[cut : cut + 8] - below(far_eta)
        seam = (seam * keep - seam_depth * rise) * seam_mask
        far_seam = (far_seam * keep - far_seam_depth * far_rise) * far_seam_mask
        v = (v * keep - mdepth * (roll(eta, -1, 0) - eta)) * mmask
        far_v = (far_v * keep - far_mdepth * (roll(far_eta, -1, 0) - far_eta)) * far_mmask
    mid = slice(rows, 2 * rows)
    surface_out[...] = eta[mid]
    transport_out[0] = u[mid]
    transport_out[1] = v[mid]

    level_row = rows_of((depth, width)).astype(F32)
    mix_rows = jnp.zeros((depth, width), F32)
    for k in range(depth):
        mix_rows = jnp.where(level_row == k, hmix[k], mix_rows)
    top, bottom = level[2 * rows - 1 : 2 * rows], level[rows : rows + 1]
    flux_top = face(
        up[flat : flat + depth],
        north_rows[0:depth],
        level_row < top,
        level_row < level[2 * rows : 2 * rows + 1],
        up[flat + depth : flat + 2 * depth],
        north_rows[depth : 2 * depth],
        mix_rows,
    )
    flux_bottom = face(
        south[flat : flat + depth],
        down[flat : flat + depth],
        level_row < level[rows - 1 : rows],
        level_row < bottom,
        south[flat + depth : flat + 2 * depth],
        down[flat + depth : flat + 2 * depth],
        mix_rows,
    )
    parts = rows // 8
    level_lane = ((lane8 & (parts * depth - 1)) // parts).astype(F32)
    mix_lanes = jnp.zeros((8, width), F32)
    for k in range(depth):
        mix_lanes = jnp.where(level_lane == k, hmix[k], mix_lanes)
    here, far_here = level[mid], far_level[mid]

    def column(x, at):
        packed = jnp.broadcast_to(x[:8, at : at + 1], (8, width))
        for i in range(1, parts):
            packed = jnp.where(lane8 % parts == i, x[8 * i : 8 * i + 8, at : at + 1], packed)
        return packed

    def side(near, beyond, level_near, level_beyond):
        return face(
            near,
            beyond,
            level_lane < level_near,
            level_lane < level_beyond,
            roll(near, -half_way, 1),
            roll(beyond, -half_way, 1),
            mix_lanes,
        )

    spot = 8 * (4 * 3 * parts // groups)
    flux_right = side(
        cols[8:16], from_east[spot : spot + 8], column(here, width - 1), column(far_here, 0)
    )
    flux_left = side(
        from_west[spot : spot + 8], cols[0:8], column(far_here, width - 1), column(here, 0)
    )

    lane = lanes_of((rows, width))
    row = rows_of((rows, width))

    def spread(x, k):
        return jnp.concatenate(
            [jnp.broadcast_to(x[:, parts * k + i : parts * k + i + 1], (8, width)) for i in range(parts)],
            axis=0,
        )

    sweep = None
    for k in range(depth):
        lateral = jnp.where(lane == width - 1, spread(flux_right, k), 0.0)
        lateral = lateral - jnp.where(lane == 0, spread(flux_left, k), 0.0)
        lateral = lateral + jnp.where(row == rows - 1, flux_top[k : k + 1], 0.0)
        lateral = lateral - jnp.where(row == 0, flux_bottom[k : k + 1], 0.0)
        stepped = jnp.where(here > k, inner[k] + lateral, 0.0)
        reduced = stepped * inverses[k]
        sweep = reduced if k == 0 else reduced + carries[k - 1] * sweep
        tracer_out[k] = sweep
    solved = sweep
    for k in range(depth - 2, -1, -1):
        solved = tracer_out[k] - primes[k] * solved
        tracer_out[k] = solved


def shards(
    tracer, velocity, surface, transport, horiz_mixing, vert_mixing, levels, land_tiles, fold_pair,
    *, n_lon, n_lat, interpret,
):
    depth, rows, width = tracer.shape
    smem = pl.BlockSpec(memory_space=pltpu.SMEM)
    vmem = pl.BlockSpec(memory_space=pltpu.VMEM)
    call = functools.partial(pl.pallas_call, interpret=interpret)

    def like(*shape):
        return jax.ShapeDtypeStruct(shape, F32)

    def on_chip(*shape):
        return like(*shape) if interpret else pltpu.VMEM(shape, F32)

    def held(x):
        return x if interpret else pltpu.with_memory_space_constraint(x, pltpu.VMEM)

    stack = 4 * rows + 2 * depth
    up, down, cols = call(
        pack_kernel,
        out_shape=(on_chip(stack, width), on_chip(stack, width), on_chip(16, width)),
        in_specs=[vmem] * 6,
        out_specs=(vmem,) * 3,
        name="pack",
    )(land_tiles, tracer, velocity, surface, transport, levels)

    south = lax.ppermute(up, "lat", [(i, i + 1) for i in range(n_lat - 1)])
    north = lax.ppermute(down, "lat", [(i + 1, i) for i in range(n_lat - 1)])

    lon = lax.axis_index("lon")
    pivot = (fold_pair[0] + width * lon) % (width * n_lon)
    turn = pivot % width
    tile = (pivot // width - (turn < width // 2).astype(jnp.int32)) % n_lon

    def fetch(x, shift):
        routes = [(shift + 1, 0)] + [(shift - t, t) for t in range(1, n_lon - 1)]
        pairs = [(s % n_lon * n_lat + n_lat - 1, t * n_lat + n_lat - 1) for s, t in routes]
        return lax.ppermute(x, ("lon", "lat"), pairs)

    def branch(shift):
        def both(x):
            later = fetch(x, (shift - 1) % n_lon)
            return later, fetch(x, shift)

        return both

    extra, main = lax.switch(tile, [branch(shift) for shift in range(n_lon)], up)

    at_top = (lax.axis_index("lat") == n_lat - 1).astype(jnp.int32)
    lon, turn, at_top = (x.reshape(1) for x in (lon, turn, at_top))
    edge_rows = 4 * 3 * rows * EDGE // width + 8
    eastward, westward = call(
        edge_kernel,
        out_shape=(on_chip(edge_rows + stack, width), on_chip(edge_rows + 2 * stack, width)),
        in_specs=[smem] + [vmem] * 6,
        out_specs=(vmem,) * 2,
        name="edge",
    )(lon, *map(held, (up, south, north, cols, main, extra)))
    from_west = lax.ppermute(eastward, "lon", [(i, (i + 1) % n_lon) for i in range(n_lon)])
    from_east = lax.ppermute(westward, "lon", [((i + 1) % n_lon, i) for i in range(n_lon)])

    inner, inverses, carries, primes = call(
        interior_kernel,
        out_shape=(
            on_chip(depth, rows, width),
            on_chip(depth, rows, width),
            on_chip(depth - 1, rows, width),
            on_chip(depth - 1, rows, width),
        ),
        in_specs=[smem] * 2 + [vmem] * 3,
        out_specs=(vmem,) * 4,
        name="interior",
    )(horiz_mixing, vert_mixing, tracer, velocity, held(up))
    return call(
        functools.partial(final_kernel, n_lon),
        out_shape=(like(depth, rows, width), like(rows, width), like(2, rows, width)),
        in_specs=[smem] * 4 + [vmem] * 13,
        out_specs=(vmem,) * 3,
        scratch_shapes=[
            pltpu.VMEM((4 * rows, width), F32),
            pltpu.VMEM((4 * rows, width), F32),
            pltpu.VMEM((8, width), F32),
            pltpu.VMEM((8, width), F32),
            pltpu.VMEM((2 * depth, width), F32),
        ],
        name="final",
    )(
        lon, turn, at_top, horiz_mixing, *map(held, (inner, inverses, carries, primes)),
        *map(held, (up, down, south, north, cols, from_west, from_east, main, extra)),
    )


def solution(mesh, interpret=False):
    def step(*args):
        return shards(*args, n_lon=mesh.shape["lon"], n_lat=mesh.shape["lat"], interpret=interpret)

    return jax.shard_map(
        step,
        mesh=mesh,
        in_specs=(
            P("member", "lat", "lon"),
            P(None, "member", "lat", "lon"),
            P(("member", "lat"), "lon"),
            P("member", "lat", "lon"),
            P("member"),
            P("member"),
            P("lat", "lon"),
            P("lat", "lon"),
            P("lon"),
        ),
        out_specs=(
            P("member", "lat", "lon"),
            P(("member", "lat"), "lon"),
            P("member", "lat", "lon"),
        ),
        check_vma=False,
    )
```

```python
import functools

import jax
import jax.numpy as jnp
from jax import lax
from jax.experimental import pallas as pl
from jax.experimental.pallas import tpu as pltpu
from jax.sharding import PartitionSpec as P


SUB = 12
fb_step = 0.6
drag_rate = 0.02
EDGE = 16
F32 = jnp.float32


def lanes_of(shape):
    return lax.broadcasted_iota(jnp.int32, shape, 1)


def rows_of(shape):
    return lax.broadcasted_iota(jnp.int32, shape, 0)


def roll(x, shift, axis):
    return pltpu.roll(x, shift % x.shape[axis], axis)


def pack_kernel(
    n_lon, lon, land, fold_pair, tracer, velocity, surface, transport, levels, up, down, cols, where
):
    depth, rows, width = tracer.shape
    pivot = lax.rem(fold_pair[0] + width * lon[0], width * n_lon)
    turn = lax.rem(pivot, width)
    behind = jnp.where(turn < width // 2, n_lon - 1, n_lon)
    where[0] = lax.rem(lax.div(pivot, width) + behind, n_lon)
    where[1] = turn
    real = (levels[...] * (1 - land[0, 0])).astype(F32)
    for out, row in ((up, rows - 1), (down, 0)):
        out[0:rows] = surface[...]
        out[rows : 2 * rows] = transport[0]
        out[2 * rows : 3 * rows] = transport[1]
        out[3 * rows : 4 * rows] = real
        for k in range(depth):
            out[4 * rows + k : 4 * rows + k + 1] = tracer[k, row : row + 1]
            at = 4 * rows + depth + k
            out[at : at + 1] = velocity[1, k, row : row + 1]
    lane = lanes_of((8, width))
    first = jnp.zeros((8, width), F32)
    last = jnp.zeros((8, width), F32)
    spot = 0
    for field in range(2):
        for k in range(depth):
            for half in range(0, rows, 8):
                part = tracer[k, half : half + 8] if field == 0 else velocity[0, k, half : half + 8]
                first = jnp.where(lane == spot, part[:, :1], first)
                last = jnp.where(lane == spot, part[:, width - 1 :], last)
                spot += 1
    cols[0:8] = first
    cols[8:16] = last


def edge_kernel(lon, up, south, north, cols, main, extra, eastward, westward):
    rows = up.shape[0] // 8
    width = up.shape[1]
    groups = width // EDGE
    lane = lanes_of((8, width)) // EDGE
    n = 0
    east = west = None
    for field in range(4):
        for block in (south, up, north):
            for half in range(0, rows, 8):
                group = n % groups
                x = block[field * rows + half : field * rows + half + 8]
                to_east = roll(x, EDGE * group - (width - EDGE), 1)
                to_west = roll(x, EDGE * group, 1)
                if group == 0:
                    east, west = to_east, to_west
                else:
                    east = jnp.where(lane == group, to_east, east)
                    west = jnp.where(lane == group, to_west, west)
                n += 1
                if n % groups == 0:
                    at = 8 * (n // groups - 1)
                    eastward[at : at + 8] = east
                    westward[at : at + 8] = west
    at = 8 * (n // groups)
    eastward[at : at + 8] = cols[8:16]
    westward[at : at + 8] = cols[0:8]
    at, size = at + 8, main.shape[0]
    is_first = jnp.full((size, width), lon[0], jnp.int32) == 0
    eastward[at : at + size] = jnp.where(is_first, extra[...], main[...])
    westward[at : at + size] = main[...]
    westward[at + size : at + 2 * size] = extra[...]


def face(near, beyond, wet_near, wet_beyond, vel_near, vel_beyond, mixing):
    flux = mixing * (beyond - near) - 0.25 * (vel_near + vel_beyond) * (near + beyond)
    return jnp.where(jnp.logical_and(wet_near, wet_beyond), flux, 0.0)


def interior_kernel(hmix, vmix, tracer, velocity, up, inner, inverses, carries, primes):
    depth, rows, width = tracer.shape
    here = up[3 * rows : 4 * rows]
    lane = lanes_of((rows, width))
    row = rows_of((rows, width))
    here_east = roll(here, -1, 1)
    here_north = roll(here, -1, 0)
    prime = link = None
    for k in range(depth):
        field, zonal, merid = tracer[k], velocity[0, k], velocity[1, k]
        wet = here > k
        mixing = hmix[k]
        east_flux = face(
            field, roll(field, -1, 1), wet, here_east > k, zonal, roll(zonal, -1, 1), mixing
        )
        east_flux = jnp.where(lane == width - 1, 0.0, east_flux)
        north_flux = face(
            field, roll(field, -1, 0), wet, here_north > k, merid, roll(merid, -1, 0), mixing
        )
        north_flux = jnp.where(row == rows - 1, 0.0, north_flux)
        inner[k] = field + (
            (east_flux - roll(east_flux, 1, 1)) + (north_flux - roll(north_flux, 1, 0))
        )
        diagonal = jnp.ones_like(field)
        if k > 0:
            diagonal = diagonal + link
        if k < depth - 1:
            next_link = jnp.where(here > k + 1, vmix[k], 0.0)
            diagonal = diagonal + next_link
        if k > 0:
            diagonal = diagonal + link * prime
        inverse = 1.0 / diagonal
        inverses[k] = inverse
        if k > 0:
            carries[k - 1] = link * inverse
        if k < depth - 1:
            prime = -next_link * inverse
            primes[k] = prime
            link = next_link


def final_kernel(
    n_lon, lon_ref, turn_ref, top_ref, hmix, inner, inverses, carries, primes, up, down, south, north, cols, from_west, from_east, main, extra,
    tracer_out, surface_out, transport_out,
    north_own, north_far, seam_own, seam_far, north_rows,
):
    depth, rows, width = inner.shape
    groups = width // EDGE
    lane8 = lanes_of((8, width))
    half_way = width // 2
    flat = 4 * rows

    def far_tile(n):
        at, group = 8 * (n // groups), n % groups
        east = roll(from_east[at : at + 8], -EDGE * group, 1)
        west = roll(from_west[at : at + 8], (width - EDGE) - EDGE * group, 1)
        return jnp.where(lane8 < half_way, east, west)

    def far_block(field, block):
        first = (field * 3 + block) * (rows // 8)
        return jnp.concatenate([far_tile(first + i) for i in range(rows // 8)], axis=0)

    def shifted(own, far, by):
        lane = lanes_of(own.shape)
        edge = width - 1 if by < 0 else 0
        a, b = roll(own, by, 1), roll(far, by, 1)
        return jnp.where(lane == edge, b, a), jnp.where(lane == edge, a, b)

    at_top = top_ref[0] == 1

    @pl.when(jnp.logical_not(at_top))
    def _():
        north_own[...] = north[0:flat]
        for field in range(4):
            north_far[field * rows : (field + 1) * rows] = far_block(field, 2)
        seam_own[...] = roll(up[3 * rows - 8 : 3 * rows], 1, 0)
        seam_far[...] = roll(far_tile((2 * 3 + 1) * (rows // 8) + rows // 8 - 1), 1, 0)
        north_rows[...] = north[flat : flat + 2 * depth]

    @pl.when(at_top)
    def _():
        turn = turn_ref[1]
        small = jnp.full((8, width), turn, jnp.int32) < half_way
        index = (turn - lane8) & (width - 1)
        less = lane8 <= turn
        back = 7 - rows_of((8, width))

        lon = jnp.full((8, width), lon_ref[0], jnp.int32)
        is_first, is_last = lon == 0, lon == n_lon - 1
        sent = 4 * 3 * rows // groups + 8
        size = main.shape[0]

        def pulled(at):
            mine, other = main[at : at + 8], extra[at : at + 8]
            west = from_west[sent + at : sent + at + 8]
            east = from_east[sent + at : sent + at + 8]
            further = from_east[sent + size + at : sent + size + at + 8]
            g0, g1, g2 = (
                jnp.take_along_axis(x, index, axis=1, mode="promise_in_bounds")
                for x in (
                    jnp.where(is_first, mine, west),
                    jnp.where(is_last, east, jnp.where(is_first, other, mine)),
                    jnp.where(is_last, further, jnp.where(is_first, east, other)),
                )
            )
            own = jnp.where(less, jnp.where(small, g0, g1), jnp.where(small, g1, g2))
            return own, g0, g1, g2

        def turned(x):
            return jnp.take_along_axis(x, back, axis=0, mode="promise_in_bounds")

        for field in range(4):
            own, far = [], []
            for half in range(rows - 8, -8, -8):
                mine, g0, g1, g2 = pulled(field * rows + half)
                low = jnp.where(jnp.logical_and(less, small), g1, g2)
                high = jnp.where(jnp.logical_or(less, small), g0, g1)
                own.append(turned(mine))
                far.append(turned(jnp.where(lane8 < half_way, low, high)))
            own, far = jnp.concatenate(own, axis=0), jnp.concatenate(far, axis=0)
            if field == 1:
                own, far = shifted(-own, -far, -1)
            if field == 2:
                seam_own[...] = -own[:8]
                seam_far[...] = -far[:8]
                own, far = roll(-own, -1, 0), roll(-far, -1, 0)
            north_own[field * rows : (field + 1) * rows] = own
            north_far[field * rows : (field + 1) * rows] = far
        for at in range(0, 2 * depth, 8):
            north_rows[at : at + 8] = pulled(flat + at)[0]

    def window(field):
        at = slice(field * rows, (field + 1) * rows)
        own = jnp.concatenate([south[at], up[at], north_own[at]], axis=0)
        far = jnp.concatenate([far_block(field, 0), far_block(field, 1), north_far[at]], axis=0)
        return own, far

    eta, far_eta = window(0)
    u, far_u = window(1)
    v, far_v = window(2)
    level, far_level = window(3)
    seam, far_seam = seam_own[...], seam_far[...]

    def sea_of(x):
        return (x > 0).astype(F32)

    sea, far_sea = sea_of(level), sea_of(far_level)
    east_sea, east_far_sea = shifted(sea, far_sea, -1)
    east_level, east_far_level = shifted(level, far_level, -1)
    scale = 2.0 * depth
    zmask, far_zmask = sea * east_sea, far_sea * east_far_sea
    zdepth = fb_step * ((level + east_level) / scale)
    far_zdepth = fb_step * ((far_level + east_far_level) / scale)
    mmask, far_mmask = sea * roll(sea, -1, 0), far_sea * roll(far_sea, -1, 0)
    mdepth = fb_step * ((level + roll(level, -1, 0)) / scale)
    far_mdepth = fb_step * ((far_level + roll(far_level, -1, 0)) / scale)
    cut = 2 * rows

    def below(x):
        return roll(x, 1, 0)[cut : cut + 8]

    seam_mask, far_seam_mask = below(mmask), below(far_mmask)
    seam_depth, far_seam_depth = below(mdepth), below(far_mdepth)
    row8 = rows_of((8, width))

    def south_of(x, line):
        moved = roll(x, 1, 0)
        fixed = jnp.where(row8 == 0, line, moved[cut : cut + 8])
        return jnp.concatenate([moved[:cut], fixed, moved[cut + 8 :]], axis=0)

    keep = 1.0 - drag_rate
    for _ in range(SUB):
        west_u, west_far_u = shifted(u, far_u, 1)
        div = (u - west_u) + (v - south_of(v, seam))
        far_div = (far_u - west_far_u) + (far_v - south_of(far_v, far_seam))
        eta = (eta - fb_step * div) * sea
        far_eta = (far_eta - fb_step * far_div) * far_sea
        east, far_east = shifted(eta, far_eta, -1)
        u = (u * keep - zdepth * (east - eta)) * zmask
        far_u = (far_u * keep - far_zdepth * (far_east - far_eta)) * far_zmask
        rise = eta[cut : cut + 8] - below(eta)
        far_rise = far_eta[cut : cut + 8] - below(far_eta)
        seam = (seam * keep - seam_depth * rise) * seam_mask
        far_seam = (far_seam * keep - far_seam_depth * far_rise) * far_seam_mask
        v = (v * keep - mdepth * (roll(eta, -1, 0) - eta)) * mmask
        far_v = (far_v * keep - far_mdepth * (roll(far_eta, -1, 0) - far_eta)) * far_mmask
    mid = slice(rows, 2 * rows)
    surface_out[...] = eta[mid]
    transport_out[0] = u[mid]
    transport_out[1] = v[mid]

    level_row = rows_of((depth, width)).astype(F32)
    mix_rows = jnp.zeros((depth, width), F32)
    for k in range(depth):
        mix_rows = jnp.where(level_row == k, hmix[k], mix_rows)
    top, bottom = level[2 * rows - 1 : 2 * rows], level[rows : rows + 1]
    flux_top = face(
        up[flat : flat + depth],
        north_rows[0:depth],
        level_row < top,
        level_row < level[2 * rows : 2 * rows + 1],
        up[flat + depth : flat + 2 * depth],
        north_rows[depth : 2 * depth],
        mix_rows,
    )
    flux_bottom = face(
        south[flat : flat + depth],
        down[flat : flat + depth],
        level_row < level[rows - 1 : rows],
        level_row < bottom,
        south[flat + depth : flat + 2 * depth],
        down[flat + depth : flat + 2 * depth],
        mix_rows,
    )
    parts = rows // 8
    level_lane = ((lane8 & (parts * depth - 1)) // parts).astype(F32)
    mix_lanes = jnp.zeros((8, width), F32)
    for k in range(depth):
        mix_lanes = jnp.where(level_lane == k, hmix[k], mix_lanes)
    here, far_here = level[mid], far_level[mid]

    def column(x, at):
        packed = jnp.broadcast_to(x[:8, at : at + 1], (8, width))
        for i in range(1, parts):
            packed = jnp.where(lane8 % parts == i, x[8 * i : 8 * i + 8, at : at + 1], packed)
        return packed

    def side(near, beyond, level_near, level_beyond):
        return face(
            near,
            beyond,
            level_lane < level_near,
            level_lane < level_beyond,
            roll(near, -half_way, 1),
            roll(beyond, -half_way, 1),
            mix_lanes,
        )

    spot = 8 * (4 * 3 * parts // groups)
    flux_right = side(
        cols[8:16], from_east[spot : spot + 8], column(here, width - 1), column(far_here, 0)
    )
    flux_left = side(
        from_west[spot : spot + 8], cols[0:8], column(far_here, width - 1), column(here, 0)
    )

    lane = lanes_of((rows, width))
    row = rows_of((rows, width))

    def spread(x, k):
        return jnp.concatenate(
            [jnp.broadcast_to(x[:, parts * k + i : parts * k + i + 1], (8, width)) for i in range(parts)],
            axis=0,
        )

    sweep = None
    for k in range(depth):
        lateral = jnp.where(lane == width - 1, spread(flux_right, k), 0.0)
        lateral = lateral - jnp.where(lane == 0, spread(flux_left, k), 0.0)
        lateral = lateral + jnp.where(row == rows - 1, flux_top[k : k + 1], 0.0)
        lateral = lateral - jnp.where(row == 0, flux_bottom[k : k + 1], 0.0)
        stepped = jnp.where(here > k, inner[k] + lateral, 0.0)
        reduced = stepped * inverses[k]
        sweep = reduced if k == 0 else reduced + carries[k - 1] * sweep
        tracer_out[k] = sweep
    solved = sweep
    for k in range(depth - 2, -1, -1):
        solved = tracer_out[k] - primes[k] * solved
        tracer_out[k] = solved


def shards(
    tracer, velocity, surface, transport, horiz_mixing, vert_mixing, levels, land_tiles, fold_pair,
    *, n_lon, n_lat, interpret,
):
    depth, rows, width = tracer.shape
    smem = pl.BlockSpec(memory_space=pltpu.SMEM)
    vmem = pl.BlockSpec(memory_space=pltpu.VMEM)
    call = functools.partial(pl.pallas_call, interpret=interpret)
    packed = pltpu.CompilerParams()

    def like(*shape):
        return jax.ShapeDtypeStruct(shape, F32)

    def on_chip(*shape):
        return like(*shape) if interpret else pltpu.VMEM(shape, F32)

    def held(x):
        return x if interpret else pltpu.with_memory_space_constraint(x, pltpu.VMEM)

    stack = 4 * rows + 2 * depth
    lon = lax.axis_index("lon")
    place = lon.reshape(1)
    up, down, cols, where = call(
        functools.partial(pack_kernel, n_lon),
        out_shape=(
            on_chip(stack, width),
            on_chip(stack, width),
            on_chip(16, width),
            jax.ShapeDtypeStruct((2,), jnp.int32) if interpret else pltpu.SMEM((2,), jnp.int32),
        ),
        in_specs=[smem] * 3 + [vmem] * 5,
        out_specs=(vmem,) * 3 + (smem,),
        name="pack",
    )(place, land_tiles, fold_pair, tracer, velocity, surface, transport, levels)

    south = lax.ppermute(up, "lat", [(i, i + 1) for i in range(n_lat - 1)])
    north = lax.ppermute(down, "lat", [(i + 1, i) for i in range(n_lat - 1)])

    def fetch(x, shift):
        routes = [(shift + 1, 0)] + [(shift - t, t) for t in range(1, n_lon - 1)]
        pairs = [(s % n_lon * n_lat + n_lat - 1, t * n_lat + n_lat - 1) for s, t in routes]
        return lax.ppermute(x, ("lon", "lat"), pairs)

    def branch(shift):
        def both(x):
            later = fetch(x, (shift - 1) % n_lon)
            return later, fetch(x, shift)

        return both

    extra, main = lax.switch(where[0], [branch(shift) for shift in range(n_lon)], up)

    at_top = (lax.axis_index("lat") == n_lat - 1).astype(jnp.int32)
    at_top = at_top.reshape(1)
    edge_rows = 4 * 3 * rows * EDGE // width + 8
    eastward, westward = call(
        edge_kernel,
        out_shape=(on_chip(edge_rows + stack, width), on_chip(edge_rows + 2 * stack, width)),
        in_specs=[smem] + [vmem] * 6,
        out_specs=(vmem,) * 2,
        name="edge",
    )(place, *map(held, (up, south, north, cols, main, extra)))
    from_west = lax.ppermute(eastward, "lon", [(i, (i + 1) % n_lon) for i in range(n_lon)])
    from_east = lax.ppermute(westward, "lon", [((i + 1) % n_lon, i) for i in range(n_lon)])

    inner, inverses, carries, primes = call(
        interior_kernel,
        out_shape=(
            on_chip(depth, rows, width),
            on_chip(depth, rows, width),
            on_chip(depth - 1, rows, width),
            on_chip(depth - 1, rows, width),
        ),
        in_specs=[smem] * 2 + [vmem] * 3,
        out_specs=(vmem,) * 4,
        compiler_params=packed,
        name="interior",
    )(horiz_mixing, vert_mixing, tracer, velocity, held(up))
    return call(
        functools.partial(final_kernel, n_lon),
        out_shape=(like(depth, rows, width), like(rows, width), like(2, rows, width)),
        in_specs=[smem] * 4 + [vmem] * 13,
        out_specs=(vmem,) * 3,
        scratch_shapes=[
            pltpu.VMEM((4 * rows, width), F32),
            pltpu.VMEM((4 * rows, width), F32),
            pltpu.VMEM((8, width), F32),
            pltpu.VMEM((8, width), F32),
            pltpu.VMEM((2 * depth, width), F32),
        ],
        compiler_params=packed,
        name="final",
    )(
        place, where, at_top, horiz_mixing, *map(held, (inner, inverses, carries, primes)),
        *map(held, (up, down, south, north, cols, from_west, from_east, main, extra)),
    )


def solution(mesh, interpret=False):
    def step(*args):
        return shards(*args, n_lon=mesh.shape["lon"], n_lat=mesh.shape["lat"], interpret=interpret)

    return jax.shard_map(
        step,
        mesh=mesh,
        in_specs=(
            P("member", "lat", "lon"),
            P(None, "member", "lat", "lon"),
            P(("member", "lat"), "lon"),
            P("member", "lat", "lon"),
            P("member"),
            P("member"),
            P("lat", "lon"),
            P("lat", "lon"),
            P("lon"),
        ),
        out_specs=(
            P("member", "lat", "lon"),
            P(("member", "lat"), "lon"),
            P("member", "lat", "lon"),
        ),
        check_vma=False,
    )
```
